128 devices in a mesh: section: 8 (over x, core), tp: 16 (over z, y).
Axes of the slice: x: 4, y: 4, z: 4, core: 2. Of those that a mesh axis runs over, the one named last changes fastest.
Arguments:
- pending_activation: bfloat16 [8, 128, 4096], P('section'), may hold values from -6 to 6
- admissible_microbatches: bfloat16 [4, 128, 4096], P(None, None, 'tp'), may hold values from -6 to 6
- arrival_plan: int32 [4], replicated, may hold values from 0 to 3, each once
- vanished_hop: int32 [1], replicated, may hold values from 1 to 7
- query_key_value_matrices: bfloat16 [8, 4096, 3, 2048], P('section', None, None, 'tp')
- mixing_projection_matrices: bfloat16 [8, 2048, 4096], P('section', 'tp'), may hold values from -0.125 to 0.125
- normalizer_factors: bfloat16 [8, 4096], P('section'), may hold values from 0.25 to 1.75
Outputs:
- activation_later: bfloat16 [8, 128, 4096], P('section')
- standby_input: bfloat16 [8, 128, 4096], P('section', None, 'tp')
The draws below stay inside these ranges and needn't reach their ends.
Inputs may be any that keep to these rules, and one draw needn't show every extreme that they name: `vanished_hop`: the preempted section is not the first. `arrival_plan`: each micro-batch index once.
All inputs are finite; a program needn't handle non-finite values.
Results may differ from the reference program's by a relative error of at most 0.013.
Values may be sent and summed in bfloat16 or wider, within the bound.
No kernel may reach another device: no remote copies, remote signals or barrier semaphores. Data moves between devices by JAX's collectives and lax.ppermute only.
A program may use at most 64 MiB of HBM per device.

```python
import jax
import jax.numpy as jnp
from jax import lax

HIDDEN_SIZE = 4096
HEADS = 16
HD = 128
STRING_LENGTH = 128
TICKS = 3
POOL = 4
LAYER_HOPS = 8


def draw_query_key_value_matrices(key, part):
    base = jax.random.normal(key, (LAYER_HOPS, HIDDEN_SIZE, 3, HEADS * HD), jnp.float32) * HIDDEN_SIZE ** (-0.5)
    return base.astype(jnp.bfloat16)


def level_of(stream_key, dims, pieces, low, high):
    loudness = 1.0
    for position, shards_of in pieces:
        draws = jax.random.uniform(jax.random.fold_in(jax.random.fold_in(stream_key, 6), position), (shards_of,), jnp.float32, low / len(pieces), high / len(pieces))
        loudness = loudness * jnp.repeat(jnp.exp(draws), dims[position] // shards_of).reshape((-1,) + (1,) * (len(dims) - 1 - position))
    return loudness


def bell_draw(rng, dims, width, limit, cuts=(), held_as=jnp.bfloat16):
    array = jax.random.normal(rng, dims, jnp.float32) * width
    if len(cuts) > 0:
        array = level_of(rng, dims, cuts, -0.22, 0.18) * array
    return jnp.clip(array, min=-limit, max=limit).astype(held_as)


def setup_inputs(seed: int = 0) -> dict:
    arg_keys = jax.random.split(jax.random.key(seed), 8)
    pending_activation = bell_draw(arg_keys[0], (LAYER_HOPS, STRING_LENGTH, HIDDEN_SIZE), 1.0, 6.0, ((0, 8),))
    admissible_microbatches = bell_draw(arg_keys[1], (POOL, STRING_LENGTH, HIDDEN_SIZE), 1.0, 6.0, ((2, 16),))
    arrival_plan = jax.random.permutation(arg_keys[2], POOL).astype(jnp.int32)
    vanished_hop = jax.random.randint(arg_keys[3], (1,), 1, LAYER_HOPS).astype(jnp.int32)
    query_key_value_matrices = draw_query_key_value_matrices(jax.random.fold_in(arg_keys[7], 71), 0)
    mixing_projection_matrices = bell_draw(arg_keys[5], (LAYER_HOPS, HEADS * HD, HIDDEN_SIZE), (HEADS * HD) ** -0.5, 0.125, ((0, 8), (1, 16)))
    normalizer_factors = jnp.clip(1.0 + 0.15 * jax.random.normal(arg_keys[6], (LAYER_HOPS, HIDDEN_SIZE), jnp.float32), 0.25, 1.75).astype(jnp.bfloat16)
    return dict(pending_activation=pending_activation, admissible_microbatches=admissible_microbatches, arrival_plan=arrival_plan, vanished_hop=vanished_hop, query_key_value_matrices=query_key_value_matrices, mixing_projection_matrices=mixing_projection_matrices, normalizer_factors=normalizer_factors)


NORM_EPS = 1e-05

def layer_norm(x_rows, scale_row):
    widened = x_rows.astype(jnp.float32)
    row_mean = lax.optimization_barrier(jnp.mean(widened, axis=-1, keepdims=True))
    centered = widened - row_mean
    row_var = lax.optimization_barrier(jnp.mean(centered * centered, axis=-1, keepdims=True))
    return (centered * lax.rsqrt(row_var + NORM_EPS) * scale_row.astype(jnp.float32)).astype(jnp.bfloat16)

def attend(normed, w_in, w_out):
    row_count = normed.shape[0]
    col_count = w_in.shape[2]
    head_count = col_count // HD
    projected = jnp.dot(normed, w_in.reshape(w_in.shape[0], 3 * col_count), preferred_element_type=jnp.float32)
    projected = projected.astype(jnp.bfloat16).reshape(row_count, 3, head_count, HD)
    queries = projected[:, 0].astype(jnp.float32)
    key_rows = projected[:, 1].astype(jnp.float32)
    values = projected[:, 2].astype(jnp.float32)
    scores = jnp.einsum('qhd,khd->hqk', queries, key_rows) * HD ** (-0.5)
    causal = jnp.arange(row_count)[:, None] >= jnp.arange(row_count)[None, :]
    scores = jnp.where(causal[None], scores, -jnp.inf)
    row_max = lax.optimization_barrier(jnp.max(scores, axis=-1, keepdims=True))
    weights = jnp.exp(scores - row_max)
    probs = (weights / lax.optimization_barrier(jnp.sum(weights, axis=-1, keepdims=True))).astype(jnp.bfloat16)
    context = jnp.einsum('hqk,khd->qhd', probs.astype(jnp.float32), values)
    context = context.astype(jnp.bfloat16).reshape(row_count, col_count)
    return jnp.dot(context, w_out, preferred_element_type=jnp.float32)

def section_layer(x_rows, w_in, w_out, scale_row):
    branch = attend(layer_norm(x_rows, scale_row), w_in, w_out)
    return (x_rows.astype(jnp.float32) + branch).astype(jnp.bfloat16)

def reference(pending_activation, admissible_microbatches, arrival_plan, vanished_hop, query_key_value_matrices, mixing_projection_matrices, normalizer_factors):
    lost_at = vanished_hop[0]
    section_ids = jnp.arange(LAYER_HOPS)[:, None, None]
    activation_later = pending_activation
    spares = None
    for tick_index in range(TICKS):
        outputs = lax.map(lambda operands: section_layer(*operands), (activation_later, query_key_value_matrices, mixing_projection_matrices, normalizer_factors))
        if tick_index == TICKS - 1:
            spares = lax.map(lambda operands: section_layer(*operands), (outputs, jnp.roll(query_key_value_matrices, -1, axis=0), jnp.roll(mixing_projection_matrices, -1, axis=0), jnp.roll(normalizer_factors, -1, axis=0)))
            redone = lax.dynamic_index_in_dim(spares, lost_at - 1, 0, keepdims=False)
        else:
            earlier = lax.dynamic_index_in_dim(outputs, lost_at - 1, 0, keepdims=False)
            redone = section_layer(earlier, lax.dynamic_index_in_dim(query_key_value_matrices, lost_at, 0, keepdims=False), lax.dynamic_index_in_dim(mixing_projection_matrices, lost_at, 0, keepdims=False), lax.dynamic_index_in_dim(normalizer_factors, lost_at, 0, keepdims=False))
        outputs = lax.dynamic_update_index_in_dim(outputs, redone, lost_at - 1, 0)
        entering = lax.dynamic_index_in_dim(admissible_microbatches, arrival_plan[tick_index], 0, keepdims=True)
        shifted = jnp.concatenate([entering, outputs[:-1]], axis=0)
        activation_later = jnp.where(section_ids == lost_at, jnp.zeros_like(shifted), jnp.where(section_ids == lost_at + 1, redone[None], shifted))
    standby_input = jnp.roll(spares, 2, axis=0)
    return (activation_later, standby_input)
```

```python
import jax
import jax.numpy as jnp
from jax import lax
from jax.sharding import PartitionSpec as P

HD = 128
TICKS = 3
PHASES = TICKS + 2

NORM_EPS = 1e-05


def shifted(value, axis, steps):
    count = lax.axis_size(axis)
    pairs = [(source, (source + steps) % count) for source in range(count)]
    return lax.ppermute(value, axis, pairs)


def from_everyone(array, axis):
    copies = jnp.broadcast_to(array, (lax.axis_size(axis), *array.shape))
    return lax.all_to_all(copies, axis, split_axis=0, concat_axis=0, tiled=True)


def columns_at_owner(array, axis):
    count = lax.axis_size(axis)
    blocks = array.reshape(array.shape[0], count, array.shape[1] // count)
    return lax.all_to_all(jnp.moveaxis(blocks, 1, 0), axis, split_axis=0, concat_axis=0, tiled=True)


def side_by_side(blocks):
    members, rows, cols = blocks.shape
    return jnp.moveaxis(blocks, 0, 1).reshape(rows, members * cols)


def layer_norm(x_rows, scale_row):
    widened = x_rows.astype(jnp.float32)
    row_mean = jnp.mean(widened, axis=-1, keepdims=True)
    centered = widened - row_mean
    row_var = jnp.mean(centered * centered, axis=-1, keepdims=True)
    return (centered * lax.rsqrt(row_var + NORM_EPS) * scale_row.astype(jnp.float32)).astype(
        jnp.bfloat16
    )


def head_context(normed, w_in):
    rows = normed.shape[0]
    projected = jnp.dot(
        normed, w_in.reshape(w_in.shape[0], 3 * HD), preferred_element_type=jnp.float32
    ).astype(jnp.bfloat16)
    queries, keys, values = projected[:, :HD], projected[:, HD : 2 * HD], projected[:, 2 * HD :]
    scores = jnp.dot(queries, keys.T, preferred_element_type=jnp.float32) * HD ** (-0.5)
    causal = jnp.arange(rows)[:, None] >= jnp.arange(rows)[None, :]
    scores = jnp.where(causal, scores, -jnp.inf)
    weights = jnp.exp(scores - jnp.max(scores, axis=-1, keepdims=True))
    probs = (weights / jnp.sum(weights, axis=-1, keepdims=True)).astype(jnp.bfloat16)
    return jnp.dot(probs, values, preferred_element_type=jnp.float32).astype(jnp.bfloat16)


def per_device(
    pending_activation,
    admissible_microbatches,
    arrival_plan,
    vanished_hop,
    query_key_value_matrices,
    mixing_projection_matrices,
    normalizer_factors,
):
    sections = lax.axis_size("section")
    mine = lax.axis_index("section")
    breadth = pending_activation.shape[2] // lax.axis_size("tp")
    col_start = lax.axis_index("tp") * breadth
    lost = vanished_hop[0]
    w_in = query_key_value_matrices[0]
    scale_row = normalizer_factors[0]
    w_cols = columns_at_owner(mixing_projection_matrices[0], "tp")
    w_cols = w_cols.reshape(-1, breadth)

    entering = [
        lax.dynamic_index_in_dim(admissible_microbatches, arrival_plan[t], 0, keepdims=False)
        for t in range(TICKS)
    ]
    late = (lost == sections - 2) | (lost == sections - 3)
    first = mine == 0
    injected = {2: first, 3: first, 4: first & late, 5: first & ~late}
    blanked = {3: (mine == lost) & (lost == sections - 1)}

    is_lost = mine == lost
    x_full = jnp.where(is_lost, jnp.zeros_like(pending_activation[0]), pending_activation[0])
    x_sh = lax.dynamic_slice_in_dim(x_full, col_start, breadth, 1)

    before = (mine + sections - 1) % sections
    ahead = before - lost
    arrives = jnp.where(
        before == 0,
        jnp.where(late, 5, 4),
        jnp.where(ahead == 1, 2, jnp.where((ahead == 2) | (ahead == 3), 5, 4)),
    )
    behind = mine - lost
    second = jnp.where(first, ~late, (behind >= 1) & (behind <= 3))

    standby_sh = jnp.zeros_like(x_sh)
    later = None
    for phase in range(1, PHASES + 1):
        context = head_context(layer_norm(x_full, scale_row), w_in)
        heads = side_by_side(from_everyone(context, "tp"))
        branch = jnp.dot(heads, w_cols, preferred_element_type=jnp.float32)
        y_sh = (x_sh.astype(jnp.float32) + branch).astype(jnp.bfloat16)
        arrived = shifted(y_sh, "section", 1)
        standby_sh = jnp.where(arrives == phase, arrived, standby_sh)
        if phase == PHASES:
            break
        x_sh = arrived
        following = phase + 1
        if following in injected:
            plan_entry = entering[min(following - 2, TICKS - 1)]
            x_sh = jnp.where(injected[following], plan_entry, x_sh)
        if following in blanked:
            x_sh = jnp.where(blanked[following], jnp.zeros_like(x_sh), x_sh)
        x_full = side_by_side(from_everyone(x_sh, "tp"))
        if following == PHASES - 1:
            later = x_full
        if following == PHASES:
            later = jnp.where(second, x_full, later)
    later = jnp.where(is_lost, jnp.zeros_like(later), later)
    return (later[None], standby_sh[None])


def solution(mesh):
    placed = (
        P("section", None, None),
        P(None, None, "tp"),
        P(),
        P(),
        P("section", None, None, "tp"),
        P("section", "tp", None),
        P("section", None),
    )
    return jax.shard_map(
        per_device,
        mesh=mesh,
        in_specs=placed,
        out_specs=(P("section", None, None), P("section", None, "tp")),
        check_vma=False,
    )
```

```python
import jax
import jax.numpy as jnp
from jax import lax
from jax.experimental import pallas as pl
from jax.experimental.pallas import tpu as pltpu
from jax.sharding import PartitionSpec as P

HD = 128
TICKS = 3
PHASES = TICKS + 2

NORM_EPS = 1e-05
CHUNKS = 4


def shifted(value, axis, steps):
    count = lax.axis_size(axis)
    pairs = [(source, (source + steps) % count) for source in range(count)]
    return lax.ppermute(value, axis, pairs)


def exchange(blocks, axis):
    return lax.all_to_all(blocks, axis, split_axis=0, concat_axis=0, tiled=True)


def from_everyone(array, axis):
    return exchange(jnp.broadcast_to(array, (lax.axis_size(axis), *array.shape)), axis)


def side_by_side(blocks):
    members, rows, cols = blocks.shape
    return jnp.moveaxis(blocks, 0, 1).reshape(rows, members * cols)


def head_context(block_of, count, breadth, gain_ref, w_ref, normed_ref, w_vmem, sems):
    features = count * breadth
    step = features // CHUNKS
    copies = [
        pltpu.make_async_copy(w_ref.at[:, pl.ds(c * step, step), :], w_vmem.at[:, pl.ds(c * step, step), :], sems.at[c])
        for c in range(CHUNKS)
    ]
    for copy in copies:
        copy.start()
    rows = normed_ref.shape[0]

    def row_sums(values_of):
        total = jnp.zeros((rows, HD), jnp.float32)
        for b in range(count):
            value = values_of(b)
            for c in range(breadth // HD):
                total = total + value[:, c * HD : (c + 1) * HD]
        return jnp.sum(total, axis=-1, keepdims=True)

    mean = row_sums(block_of) * (1.0 / features)

    def squares(b):
        centered = block_of(b) - mean
        return centered * centered

    var = row_sums(squares) * (1.0 / features)
    scale = lax.rsqrt(var + NORM_EPS)
    for b in range(count):
        cols = pl.ds(b * breadth, breadth)
        gain = gain_ref[:, cols].astype(jnp.float32)
        normed_ref[:, cols] = ((block_of(b) - mean) * scale * gain).astype(jnp.bfloat16)
    parts = [jnp.zeros((rows, HD), jnp.float32) for _ in range(3)]
    for c in range(CHUNKS):
        copies[c].wait()
        piece = normed_ref[:, c * step : (c + 1) * step]
        for j in range(3):
            parts[j] = parts[j] + jnp.dot(
                piece, w_vmem[j, c * step : (c + 1) * step, :], preferred_element_type=jnp.float32
            )
    queries, keys, values = (part.astype(jnp.bfloat16) for part in parts)
    scores = lax.dot_general(
        queries, keys, (((1,), (1,)), ((), ())), preferred_element_type=jnp.float32
    ) * HD ** (-0.5)
    causal = lax.broadcasted_iota(jnp.int32, scores.shape, 0) >= lax.broadcasted_iota(
        jnp.int32, scores.shape, 1
    )
    scores = jnp.where(causal, scores, -jnp.inf)
    weights = jnp.exp(scores - jnp.max(scores, axis=-1, keepdims=True))
    probs = (weights / jnp.sum(weights, axis=-1, keepdims=True)).astype(jnp.bfloat16)
    return jnp.dot(probs, values, preferred_element_type=jnp.float32).astype(jnp.bfloat16)


def opening_kernel(lost_ref, x_ref, gain_ref, w_ref, mix_ref, out_ref, normed_ref, w_vmem, sems):
    count = out_ref.shape[0]
    breadth = x_ref.shape[1] // count
    dead = lost_ref[0] != 0

    def block_of(b):
        block = x_ref[:, b * breadth : (b + 1) * breadth].astype(jnp.float32)
        return jnp.where(dead, 0.0, block)

    for b in range(count):
        out_ref[b, :, :breadth] = mix_ref[:, b * breadth : (b + 1) * breadth]
    context = head_context(block_of, count, breadth, gain_ref, w_ref, normed_ref, w_vmem, sems)
    for b in range(count):
        out_ref[b, :, breadth:] = context


def phase_kernel(x_ref, gain_ref, w_ref, out_ref, normed_ref, w_vmem, sems):
    count, _, breadth = x_ref.shape
    context = head_context(
        lambda b: x_ref[b].astype(jnp.float32), count, breadth, gain_ref, w_ref, normed_ref, w_vmem, sems
    )
    for b in range(count):
        out_ref[b] = context


def mix_kernel(x_ref, heads_ref, mixed_ref, out_ref):
    count, _, breadth = mixed_ref.shape[0], mixed_ref.shape[1], x_ref.shape[1]
    start = heads_ref.shape[2] - HD
    branch = jnp.zeros(x_ref.shape, jnp.float32)
    for h in range(count):
        branch = branch + jnp.dot(
            heads_ref[h, :, start:], mixed_ref[h, :, :breadth], preferred_element_type=jnp.float32
        )
    out_ref[...] = (x_ref[...].astype(jnp.float32) + branch).astype(jnp.bfloat16)


VMEM = pl.BlockSpec(memory_space=pltpu.VMEM)
SMEM = pl.BlockSpec(memory_space=pltpu.SMEM)
ANY = pl.BlockSpec(memory_space=pl.ANY)
LIMIT = pltpu.CompilerParams(vmem_limit_bytes=24 * 1024 * 1024)


def scratch(rows, features):
    return [
        pltpu.VMEM((rows, features), jnp.bfloat16),
        pltpu.VMEM((3, features, HD), jnp.bfloat16),
        pltpu.SemaphoreType.DMA((CHUNKS,)),
    ]


def opening(dead, x_full, gain, w_in, mixing, members):
    rows, features = x_full.shape
    return pl.pallas_call(
        opening_kernel,
        out_shape=jax.ShapeDtypeStruct((members, rows, features // members + HD), jnp.bfloat16),
        in_specs=[SMEM, VMEM, VMEM, ANY, VMEM],
        out_specs=VMEM,
        scratch_shapes=scratch(rows, features),
        compiler_params=LIMIT,
        name="opening",
    )(dead, x_full, gain, w_in, mixing)


def contexts(x_blocks, gain, w_in):
    members, rows, breadth = x_blocks.shape
    return pl.pallas_call(
        phase_kernel,
        out_shape=jax.ShapeDtypeStruct((members, rows, HD), jnp.bfloat16),
        in_specs=[VMEM, VMEM, ANY],
        out_specs=VMEM,
        scratch_shapes=scratch(rows, members * breadth),
        compiler_params=LIMIT,
        name="contexts",
    )(x_blocks, gain, w_in)


def mixed_rows(x_sh, heads, mixed):
    return pl.pallas_call(
        mix_kernel,
        out_shape=jax.ShapeDtypeStruct(x_sh.shape, jnp.bfloat16),
        in_specs=[VMEM, VMEM, VMEM],
        out_specs=VMEM,
        compiler_params=LIMIT,
        name="mixed_rows",
    )(x_sh, heads, mixed)


def per_device(
    pending_activation,
    admissible_microbatches,
    arrival_plan,
    vanished_hop,
    query_key_value_matrices,
    mixing_projection_matrices,
    normalizer_factors,
):
    sections = lax.axis_size("section")
    mine = lax.axis_index("section")
    members = lax.axis_size("tp")
    breadth = pending_activation.shape[2] // members
    col_start = lax.axis_index("tp") * breadth
    lost = vanished_hop[0]
    w_in = jnp.moveaxis(query_key_value_matrices[0], 1, 0)

    entering = [
        lax.dynamic_index_in_dim(admissible_microbatches, arrival_plan[t], 0, keepdims=False)
        for t in range(TICKS)
    ]
    late = (lost == sections - 2) | (lost == sections - 3)
    first = mine == 0
    injected = {2: first, 3: first, 4: first & late, 5: first & ~late}
    blanked = {3: (mine == lost) & (lost == sections - 1)}

    is_lost = mine == lost
    before = (mine + sections - 1) % sections
    ahead = before - lost
    arrives = jnp.where(
        before == 0,
        jnp.where(late, 5, 4),
        jnp.where(ahead == 1, 2, jnp.where((ahead == 2) | (ahead == 3), 5, 4)),
    )
    behind = mine - lost
    second = jnp.where(first, ~late, (behind >= 1) & (behind <= 3))

    x_sh = lax.dynamic_slice_in_dim(pending_activation[0], col_start, breadth, 1)
    x_sh = jnp.where(is_lost, jnp.zeros_like(x_sh), x_sh)
    dead = is_lost.astype(jnp.int32)[None]
    sent = opening(
        dead, pending_activation[0], normalizer_factors, w_in, mixing_projection_matrices[0], members
    )
    mixed = exchange(sent, "tp")
    heads = mixed

    standby_sh = jnp.zeros_like(x_sh)
    fourth = None
    for phase in range(1, PHASES + 1):
        y_sh = mixed_rows(x_sh, heads, mixed)
        arrived = shifted(y_sh, "section", 1)
        standby_sh = jnp.where(arrives == phase, arrived, standby_sh)
        if phase == PHASES:
            break
        x_sh = arrived
        following = phase + 1
        if following in injected:
            plan_entry = entering[min(following - 2, TICKS - 1)]
            x_sh = jnp.where(injected[following], plan_entry, x_sh)
        if following in blanked:
            x_sh = jnp.where(blanked[following], jnp.zeros_like(x_sh), x_sh)
        x_blocks = from_everyone(x_sh, "tp")
        if following == PHASES - 1:
            fourth = x_blocks
        heads = exchange(contexts(x_blocks, normalizer_factors, w_in), "tp")
    later = side_by_side(jnp.where(second, x_blocks, fourth))
    later = jnp.where(is_lost, jnp.zeros_like(later), later)
    return (later[None], standby_sh[None])


def solution(mesh):
    placed = (
        P("section", None, None),
        P(None, None, "tp"),
        P(),
        P(),
        P("section", None, None, "tp"),
        P("section", "tp", None),
        P("section", None),
    )
    return jax.shard_map(
        per_device,
        mesh=mesh,
        in_specs=placed,
        out_specs=(P("section", None, None), P("section", None, "tp")),
        check_vma=False,
    )
```

```python
import jax
import jax.numpy as jnp
from jax import lax
from jax.experimental import pallas as pl
from jax.experimental.pallas import tpu as pltpu
from jax.sharding import PartitionSpec as P

HD = 128
TICKS = 3
PHASES = TICKS + 2

NORM_EPS = 1e-05
CHUNKS = 4


def shifted(value, axis, steps):
    count = lax.axis_size(axis)
    pairs = [(source, (source + steps) % count) for source in range(count)]
    return lax.ppermute(value, axis, pairs)


def moved(value, axis, parity):
    count = lax.axis_size(axis)
    pairs = [((target - 2) % count, target) for target in range(count) if target % 2 == parity]
    return lax.ppermute(value, axis, pairs)


def swapped(value, axis):
    return lax.ppermute(value, axis, [(s, s + 1 - 2 * (s % 2)) for s in range(lax.axis_size(axis))])


def exchange(blocks, axis):
    return lax.all_to_all(blocks, axis, split_axis=0, concat_axis=0, tiled=True)


def from_everyone(array, axis):
    return exchange(jnp.broadcast_to(array, (lax.axis_size(axis), *array.shape)), axis)


def side_by_side(blocks):
    members, rows, cols = blocks.shape
    return jnp.moveaxis(blocks, 0, 1).reshape(rows, members * cols)


def head_context(block_of, count, breadth, gain_ref, weights_of, normed_ref):
    features = count * breadth
    step = features // CHUNKS
    rows = normed_ref.shape[0]

    def row_sums(values_of):
        total = jnp.zeros((rows, HD), jnp.float32)
        for b in range(count):
            value = values_of(b)
            for c in range(breadth // HD):
                total = total + value[:, c * HD : (c + 1) * HD]
        return jnp.sum(total, axis=-1, keepdims=True)

    mean = row_sums(block_of) * (1.0 / features)

    def squares(b):
        centered = block_of(b) - mean
        return centered * centered

    var = row_sums(squares) * (1.0 / features)
    scale = lax.rsqrt(var + NORM_EPS)
    for b in range(count):
        cols = pl.ds(b * breadth, breadth)
        gain = gain_ref[:, cols].astype(jnp.float32)
        normed_ref[:, cols] = ((block_of(b) - mean) * scale * gain).astype(jnp.bfloat16)
    parts = [jnp.zeros((rows, HD), jnp.float32) for _ in range(3)]
    for c in range(CHUNKS):
        piece = normed_ref[:, c * step : (c + 1) * step]
        w_ref = weights_of(c)
        for j in range(3):
            parts[j] = parts[j] + jnp.dot(
                piece, w_ref[j, c * step : (c + 1) * step, :], preferred_element_type=jnp.float32
            )
    queries, keys, values = (part.astype(jnp.bfloat16) for part in parts)
    scores = lax.dot_general(
        queries, keys, (((1,), (1,)), ((), ())), preferred_element_type=jnp.float32
    ) * HD ** (-0.5)
    causal = lax.broadcasted_iota(jnp.int32, scores.shape, 0) >= lax.broadcasted_iota(
        jnp.int32, scores.shape, 1
    )
    scores = jnp.where(causal, scores, -jnp.inf)
    weights = jnp.exp(scores - jnp.max(scores, axis=-1, keepdims=True))
    probs = (weights / jnp.sum(weights, axis=-1, keepdims=True)).astype(jnp.bfloat16)
    return jnp.dot(probs, values, preferred_element_type=jnp.float32).astype(jnp.bfloat16)


def opening_kernel(dead_ref, x_hbm, gain_ref, w_hbm, mix_hbm, out_ref, x_ref, normed_ref, w_ref, x_sem, w_sems, mix_sems):
    count = out_ref.shape[0]
    rows, features = x_ref.shape
    breadth = features // count
    step = features // CHUNKS
    x_copy = pltpu.make_async_copy(x_hbm, x_ref, x_sem.at[0])
    w_copies = [
        pltpu.make_async_copy(
            w_hbm.at[:, pl.ds(c * step, step), :], w_ref.at[:, pl.ds(c * step, step), :], w_sems.at[c]
        )
        for c in range(CHUNKS)
    ]
    mix_copies = [
        pltpu.make_async_copy(
            mix_hbm.at[:, pl.ds(b * breadth, breadth)], out_ref.at[b, :, pl.ds(0, breadth)], mix_sems.at[b]
        )
        for b in range(count)
    ]
    for copy in [x_copy, *w_copies, *mix_copies]:
        copy.start()
    dead = dead_ref[0] != 0

    def block_of(b):
        block = x_ref[:, b * breadth : (b + 1) * breadth].astype(jnp.float32)
        return jnp.where(dead, 0.0, block)

    def weights_of(c):
        w_copies[c].wait()
        return w_ref

    x_copy.wait()
    context = head_context(block_of, count, breadth, gain_ref, weights_of, normed_ref)
    for b in range(count):
        out_ref[b, :, breadth:] = context
    for copy in mix_copies:
        copy.wait()


def phase_kernel(x_ref, gain_ref, w_ref, out_ref, normed_ref):
    count, _, breadth = x_ref.shape
    context = head_context(
        lambda b: x_ref[b].astype(jnp.float32), count, breadth, gain_ref, lambda c: w_ref, normed_ref
    )
    for b in range(count):
        out_ref[b] = context


def mix_kernel(x_ref, heads_ref, mixed_ref, out_ref):
    count, _, breadth = mixed_ref.shape[0], mixed_ref.shape[1], x_ref.shape[1]
    start = heads_ref.shape[2] - HD
    branch = jnp.zeros(x_ref.shape, jnp.float32)
    for h in range(count):
        branch = branch + jnp.dot(
            heads_ref[h, :, start:], mixed_ref[h, :, :breadth], preferred_element_type=jnp.float32
        )
    out_ref[...] = (x_ref[...].astype(jnp.float32) + branch).astype(jnp.bfloat16)


VMEM = pl.BlockSpec(memory_space=pltpu.VMEM)
SMEM = pl.BlockSpec(memory_space=pltpu.SMEM)
HBM = pl.BlockSpec(memory_space=pltpu.HBM)
LIMIT = pltpu.CompilerParams(vmem_limit_bytes=24 * 1024 * 1024)


def opening(dead, x_full, gain, w_in, mixing, members):
    rows, features = x_full.shape
    return pl.pallas_call(
        opening_kernel,
        out_shape=jax.ShapeDtypeStruct((members, rows, features // members + HD), jnp.bfloat16),
        in_specs=[SMEM, HBM, VMEM, HBM, HBM],
        out_specs=VMEM,
        scratch_shapes=[
            pltpu.VMEM((rows, features), jnp.bfloat16),
            pltpu.VMEM((rows, features), jnp.bfloat16),
            pltpu.VMEM((3, features, HD), jnp.bfloat16),
            pltpu.SemaphoreType.DMA((1,)),
            pltpu.SemaphoreType.DMA((CHUNKS,)),
            pltpu.SemaphoreType.DMA((members,)),
        ],
        compiler_params=LIMIT,
        name="opening",
    )(dead, x_full, gain, w_in, mixing)


def contexts(x_blocks, gain, w_in):
    members, rows, breadth = x_blocks.shape
    return pl.pallas_call(
        phase_kernel,
        out_shape=jax.ShapeDtypeStruct((members, rows, HD), jnp.bfloat16),
        in_specs=[VMEM, VMEM, VMEM],
        out_specs=VMEM,
        scratch_shapes=[pltpu.VMEM((rows, members * breadth), jnp.bfloat16)],
        compiler_params=LIMIT,
        name="contexts",
    )(x_blocks, gain, w_in)


def mixed_rows(x_sh, heads, mixed):
    return pl.pallas_call(
        mix_kernel,
        out_shape=jax.ShapeDtypeStruct(x_sh.shape, jnp.bfloat16),
        in_specs=[VMEM, VMEM, VMEM],
        out_specs=VMEM,
        compiler_params=LIMIT,
        name="mixed_rows",
    )(x_sh, heads, mixed)


def per_device(
    pending_activation,
    admissible_microbatches,
    arrival_plan,
    vanished_hop,
    query_key_value_matrices,
    mixing_projection_matrices,
    normalizer_factors,
):
    sections = lax.axis_size("section")
    mine = lax.axis_index("section")
    members = lax.axis_size("tp")
    breadth = pending_activation.shape[2] // members
    col_start = lax.axis_index("tp") * breadth
    lost = vanished_hop[0]
    w_in = jnp.moveaxis(query_key_value_matrices[0], 1, 0)

    gain = normalizer_factors

    entering = [
        lax.dynamic_index_in_dim(admissible_microbatches, arrival_plan[t], 0, keepdims=False)
        for t in range(TICKS)
    ]
    late = (lost == sections - 2) | (lost == sections - 3)
    first = mine == 0
    odd = mine % 2 == 1
    other_first = mine == 1
    injected = {2: other_first, 3: first, 4: other_first & late, 5: first & ~late}
    blanked = {3: (mine == lost) & (lost == sections - 1)}

    is_lost = mine == lost
    before = (mine + sections - 1) % sections
    ahead = before - lost
    arrives = jnp.where(
        before == 0,
        jnp.where(late, 5, 4),
        jnp.where(ahead == 1, 2, jnp.where((ahead == 2) | (ahead == 3), 5, 4)),
    )
    behind = mine - lost
    second = jnp.where(first, ~late, (behind >= 1) & (behind <= 3))

    x_sh = lax.dynamic_slice_in_dim(pending_activation[0], col_start, breadth, 1)
    x_sh = jnp.where(is_lost, jnp.zeros_like(x_sh), x_sh)
    dead = is_lost.astype(jnp.int32)[None]
    other_w, other_gain = swapped(w_in, "section"), swapped(gain, "section")
    sent = opening(dead, pending_activation[0], gain, w_in, mixing_projection_matrices[0], members)
    mixed = exchange(sent, "tp")
    other_mixed = swapped(mixed, "section")
    heads = mixed

    standby_sh = jnp.zeros_like(x_sh)
    fourth = None
    for phase in range(1, PHASES):
        y_sh = mixed_rows(x_sh, heads, mixed if phase % 2 == 1 else other_mixed)
        parity = phase % 2
        arrived = jnp.where(odd == (parity == 1), moved(y_sh, "section", parity), y_sh)
        if phase % 2 == 0:
            standby_sh = jnp.where(arrives == phase, arrived, standby_sh)
        x_sh = arrived
        following = phase + 1
        plan_entry = entering[min(following - 2, TICKS - 1)]
        x_sh = jnp.where(injected[following], plan_entry, x_sh)
        if following in blanked:
            x_sh = jnp.where(blanked[following], jnp.zeros_like(x_sh), x_sh)
        x_blocks = from_everyone(x_sh, "tp")
        if following == PHASES - 1:
            fourth = swapped(x_blocks, "section")
        weights = (gain, w_in) if following % 2 == 1 else (other_gain, other_w)
        heads = exchange(contexts(x_blocks, *weights), "tp")
    y_sh = mixed_rows(x_sh, heads, mixed)
    y_sh, x_blocks, fourth = lax.optimization_barrier((y_sh, x_blocks, fourth))
    arrived = shifted(y_sh, "section", 1)
    standby_sh = jnp.where(arrives == PHASES, arrived, standby_sh)
    later = side_by_side(jnp.where(second, x_blocks, fourth))
    later = jnp.where(is_lost, jnp.zeros_like(later), later)
    return (later[None], standby_sh[None])


def solution(mesh):
    placed = (
        P("section", None, None),
        P(None, None, "tp"),
        P(),
        P(),
        P("section", None, None, "tp"),
        P("section", "tp", None),
        P("section", None),
    )
    return jax.shard_map(
        per_device,
        mesh=mesh,
        in_specs=placed,
        out_specs=(P("section", None, None), P("section", None, "tp")),
        check_vma=False,
    )
```

```python
import jax
import jax.numpy as jnp
from jax import lax
from jax.experimental import pallas as pl
from jax.experimental.pallas import tpu as pltpu
from jax.sharding import PartitionSpec as P

HD = 128
TICKS = 3
PHASES = TICKS + 2

NORM_EPS = 1e-05
CHUNKS = 4


def shifted(value, axis, steps):
    count = lax.axis_size(axis)
    pairs = [(source, (source + steps) % count) for source in range(count)]
    return lax.ppermute(value, axis, pairs)


def moved(value, axis, parity):
    count = lax.axis_size(axis)
    pairs = [((target - 2) % count, target) for target in range(count) if target % 2 == parity]
    return lax.ppermute(value, axis, pairs)


def swapped(value, axis):
    return lax.ppermute(value, axis, [(s, s + 1 - 2 * (s % 2)) for s in range(lax.axis_size(axis))])


def exchange(blocks, axis):
    return lax.all_to_all(blocks, axis, split_axis=0, concat_axis=0, tiled=True)


def from_everyone(array, axis):
    return exchange(jnp.broadcast_to(array, (lax.axis_size(axis), *array.shape)), axis)


def side_by_side(blocks):
    members, rows, cols = blocks.shape
    return jnp.moveaxis(blocks, 0, 1).reshape(rows, members * cols)


def head_context(block_of, count, breadth, gain_of, weights_of, normed_ref):
    features = count * breadth
    step = features // CHUNKS
    rows = normed_ref.shape[0]

    def row_sums(values_of):
        total = jnp.zeros((rows, HD), jnp.float32)
        for b in range(count):
            value = values_of(b)
            for c in range(breadth // HD):
                total = total + value[:, c * HD : (c + 1) * HD]
        return jnp.sum(total, axis=-1, keepdims=True)

    mean = row_sums(block_of) * (1.0 / features)

    def squares(b):
        centered = block_of(b) - mean
        return centered * centered

    var = row_sums(squares) * (1.0 / features)
    scale = lax.rsqrt(var + NORM_EPS)
    for b in range(count):
        gain = gain_of(b).astype(jnp.float32)
        normed_ref[:, b * breadth : (b + 1) * breadth] = ((block_of(b) - mean) * scale * gain).astype(
            jnp.bfloat16
        )
    parts = [jnp.zeros((rows, HD), jnp.float32) for _ in range(3)]
    for c in range(CHUNKS):
        piece = normed_ref[:, c * step : (c + 1) * step]
        w_ref = weights_of(c)
        for j in range(3):
            parts[j] = parts[j] + jnp.dot(
                piece, w_ref[j, c * step : (c + 1) * step, :], preferred_element_type=jnp.float32
            )
    queries, keys, values = (part.astype(jnp.bfloat16) for part in parts)
    scores = lax.dot_general(
        queries, keys, (((1,), (1,)), ((), ())), preferred_element_type=jnp.float32
    ) * HD ** (-0.5)
    causal = lax.broadcasted_iota(jnp.int32, scores.shape, 0) >= lax.broadcasted_iota(
        jnp.int32, scores.shape, 1
    )
    scores = jnp.where(causal, scores, -jnp.inf)
    weights = jnp.exp(scores - jnp.max(scores, axis=-1, keepdims=True))
    probs = (weights / jnp.sum(weights, axis=-1, keepdims=True)).astype(jnp.bfloat16)
    return jnp.dot(probs, values, preferred_element_type=jnp.float32).astype(jnp.bfloat16)


def opening_kernel(
    dead_ref, x_hbm, gain_hbm, w_hbm, mix_hbm, out_ref, x_ref, gain_ref, normed_ref, w_ref, sems, w_sems, mix_sems
):
    count = out_ref.shape[0]
    rows, features = x_ref.shape
    breadth = features // count
    step = features // CHUNKS
    x_copy = pltpu.make_async_copy(x_hbm, x_ref, sems.at[0])
    gain_copy = pltpu.make_async_copy(gain_hbm, gain_ref, sems.at[1])
    w_copies = [
        pltpu.make_async_copy(
            w_hbm.at[:, pl.ds(c * step, step), :], w_ref.at[:, pl.ds(c * step, step), :], w_sems.at[c]
        )
        for c in range(CHUNKS)
    ]
    mix_copies = [
        pltpu.make_async_copy(
            mix_hbm.at[:, pl.ds(b * breadth, breadth)], out_ref.at[b, :, pl.ds(0, breadth)], mix_sems.at[b]
        )
        for b in range(count)
    ]
    for copy in [x_copy, gain_copy, *w_copies, *mix_copies]:
        copy.start()
    dead = dead_ref[0] != 0

    def block_of(b):
        block = x_ref[:, b * breadth : (b + 1) * breadth].astype(jnp.float32)
        return jnp.where(dead, 0.0, block)

    def weights_of(c):
        w_copies[c].wait()
        return w_ref

    def gain_of(b):
        return gain_ref[:, b * breadth : (b + 1) * breadth]

    x_copy.wait()
    gain_copy.wait()
    context = head_context(block_of, count, breadth, gain_of, weights_of, normed_ref)
    for b in range(count):
        out_ref[b, :, breadth:] = context
    for copy in mix_copies:
        copy.wait()


def phase_kernel(x_ref, pack_ref, w_ref, out_ref, normed_ref):
    count, _, breadth = x_ref.shape

    def gain_of(b):
        return pack_ref[count, b : b + 1, :]

    context = head_context(
        lambda b: x_ref[b].astype(jnp.float32), count, breadth, gain_of, lambda c: w_ref, normed_ref
    )
    for b in range(count):
        out_ref[b] = context


def mix_kernel(x_ref, heads_ref, mixed_ref, out_ref):
    branch = jnp.zeros(x_ref.shape, jnp.float32)
    for h in range(heads_ref.shape[0]):
        branch = branch + jnp.dot(heads_ref[h], mixed_ref[h], preferred_element_type=jnp.float32)
    out_ref[...] = (x_ref[...].astype(jnp.float32) + branch).astype(jnp.bfloat16)


def first_mix_kernel(x_ref, joint_ref, gain_ref, out_ref, pack_ref):
    count, breadth = joint_ref.shape[0], x_ref.shape[1]
    branch = jnp.zeros(x_ref.shape, jnp.float32)
    for h in range(count):
        branch = branch + jnp.dot(
            joint_ref[h, :, breadth:], joint_ref[h, :, :breadth], preferred_element_type=jnp.float32
        )
    out_ref[...] = (x_ref[...].astype(jnp.float32) + branch).astype(jnp.bfloat16)
    for h in range(count):
        pack_ref[h] = joint_ref[h, :, :breadth]
    pack_ref[count] = jnp.zeros(x_ref.shape, jnp.bfloat16)
    pack_ref[count, :count] = gain_ref[...]


VMEM = pl.BlockSpec(memory_space=pltpu.VMEM)
SMEM = pl.BlockSpec(memory_space=pltpu.SMEM)
HBM = pl.BlockSpec(memory_space=pltpu.HBM)
LIMIT = pltpu.CompilerParams(vmem_limit_bytes=16 * 1024 * 1024)
WHOLE = pltpu.CompilerParams(vmem_limit_bytes=63 * 1024 * 1024)


def opening(dead, x_full, gain, w_in, mixing, members):
    rows, features = x_full.shape
    return pl.pallas_call(
        opening_kernel,
        out_shape=jax.ShapeDtypeStruct((members, rows, features // members + HD), jnp.bfloat16),
        in_specs=[SMEM, HBM, HBM, HBM, HBM],
        out_specs=VMEM,
        scratch_shapes=[
            pltpu.VMEM((rows, features), jnp.bfloat16),
            pltpu.VMEM((1, features), jnp.bfloat16),
            pltpu.VMEM((rows, features), jnp.bfloat16),
            pltpu.VMEM((3, features, HD), jnp.bfloat16),
            pltpu.SemaphoreType.DMA((2,)),
            pltpu.SemaphoreType.DMA((CHUNKS,)),
            pltpu.SemaphoreType.DMA((members,)),
        ],
        compiler_params=WHOLE,
        name="opening",
    )(dead, x_full, gain, w_in, mixing)


def contexts(x_blocks, pack, w_in):
    members, rows, breadth = x_blocks.shape
    return pl.pallas_call(
        phase_kernel,
        out_shape=jax.ShapeDtypeStruct((members, rows, HD), jnp.bfloat16),
        in_specs=[VMEM, VMEM, VMEM],
        out_specs=VMEM,
        scratch_shapes=[pltpu.VMEM((rows, members * breadth), jnp.bfloat16)],
        compiler_params=LIMIT,
        name="contexts",
    )(x_blocks, pack, w_in)


def mixed_rows(x_sh, heads, mixed):
    return pl.pallas_call(
        mix_kernel,
        out_shape=jax.ShapeDtypeStruct(x_sh.shape, jnp.bfloat16),
        in_specs=[VMEM, VMEM, VMEM],
        out_specs=VMEM,
        compiler_params=LIMIT,
        name="mixed_rows",
    )(x_sh, heads, mixed)


def first_mixed_rows(x_sh, joint, gain):
    members, rows, _ = joint.shape
    return pl.pallas_call(
        first_mix_kernel,
        out_shape=[
            jax.ShapeDtypeStruct(x_sh.shape, jnp.bfloat16),
            jax.ShapeDtypeStruct((members + 1, rows, x_sh.shape[1]), jnp.bfloat16),
        ],
        in_specs=[VMEM, VMEM, VMEM],
        out_specs=[VMEM, VMEM],
        compiler_params=LIMIT,
        name="first_mixed_rows",
    )(x_sh, joint, gain)


def per_device(
    pending_activation,
    admissible_microbatches,
    arrival_plan,
    vanished_hop,
    query_key_value_matrices,
    mixing_projection_matrices,
    normalizer_factors,
):
    sections = lax.axis_size("section")
    mine = lax.axis_index("section")
    members = lax.axis_size("tp")
    breadth = pending_activation.shape[2] // members
    col_start = lax.axis_index("tp") * breadth
    lost = vanished_hop[0]
    w_in = jnp.moveaxis(query_key_value_matrices[0], 1, 0)

    gain = normalizer_factors

    late = (lost == sections - 2) | (lost == sections - 3)
    first = mine == 0
    odd = mine % 2 == 1
    other_first = mine == 1
    is_lost = mine == lost
    before = (mine + sections - 1) % sections
    ahead = before - lost
    arrives = jnp.where(
        before == 0,
        jnp.where(late, 5, 4),
        jnp.where(ahead == 1, 2, jnp.where((ahead == 2) | (ahead == 3), 5, 4)),
    )
    behind = mine - lost
    second = jnp.where(first, ~late, (behind >= 1) & (behind <= 3))

    entering = [
        lax.dynamic_index_in_dim(admissible_microbatches, arrival_plan[t], 0, keepdims=False)
        for t in range(TICKS)
    ]
    x_sh = lax.dynamic_slice_in_dim(pending_activation[0], col_start, breadth, 1)
    x_sh = jnp.where(is_lost, jnp.zeros_like(x_sh), x_sh)
    dead = is_lost.astype(jnp.int32)[None]
    sent = opening(dead, pending_activation[0], gain, w_in, mixing_projection_matrices[0], members)
    gain = gain.reshape(members, breadth)
    flags = [odd, is_lost, second, first, other_first, first & late, other_first & late, first & ~late]
    flags += [is_lost & (lost == sections - 1), arrives == 2, arrives == 4, arrives == 5]
    sent, x_sh, gain, entering, flags = lax.optimization_barrier((sent, x_sh, gain, entering, flags))
    odd, is_lost, second, first, other_first, first_late, other_late, first_soon, blank, *arriving = flags
    injected = {2: other_first, 3: first, 4: other_late, 5: first_soon}

    y_sh, pack = first_mixed_rows(x_sh, exchange(sent, "tp"), gain)
    pack, leaving_w = lax.optimization_barrier((pack, w_in))
    other_pack, other_w = swapped(pack, "section"), swapped(leaving_w, "section")

    standby_sh = None
    for phase in range(1, PHASES):
        parity = phase % 2
        arrived = jnp.where(odd == (parity == 1), moved(y_sh, "section", parity), y_sh)
        if phase == 2:
            standby_sh = jnp.where(arriving[0], arrived, jnp.zeros_like(arrived))
        if phase == 4:
            standby_sh = jnp.where(arriving[1], arrived, standby_sh)
        following = phase + 1
        x_sh = jnp.where(injected[following], entering[min(following - 2, TICKS - 1)], arrived)
        if following == 3:
            x_sh = jnp.where(blank, jnp.zeros_like(x_sh), x_sh)
        if following == PHASES:
            x_sh, standby_sh, fourth = lax.optimization_barrier((x_sh, standby_sh, fourth))
        elif standby_sh is not None:
            x_sh, standby_sh = lax.optimization_barrier((x_sh, standby_sh))
        x_blocks = from_everyone(x_sh, "tp")
        if following == PHASES - 1:
            fourth = swapped(x_blocks, "section")
        layer_w, layer_pack = (w_in, pack) if following % 2 == 1 else (other_w, other_pack)
        heads = exchange(contexts(x_blocks, layer_pack, layer_w), "tp")
        y_sh = mixed_rows(x_sh, heads, layer_pack)
    y_sh, x_blocks, fourth = lax.optimization_barrier((y_sh, x_blocks, fourth))
    arrived = shifted(y_sh, "section", 1)
    standby_sh = jnp.where(arriving[2], arrived, standby_sh)
    later = side_by_side(jnp.where(second, x_blocks, fourth))
    later = jnp.where(is_lost, jnp.zeros_like(later), later)
    return (later[None], standby_sh[None])


def solution(mesh):
    placed = (
        P("section", None, None),
        P(None, None, "tp"),
        P(),
        P(),
        P("section", None, None, "tp"),
        P("section", "tp", None),
        P("section", None),
    )
    return jax.shard_map(
        per_device,
        mesh=mesh,
        in_specs=placed,
        out_specs=(P("section", None, None), P("section", None, "tp")),
        check_vma=False,
    )
```

```python
import jax
import jax.numpy as jnp
from jax import lax
from jax.experimental import pallas as pl
from jax.experimental.pallas import tpu as pltpu
from jax.sharding import PartitionSpec as P

HD = 128
TICKS = 3
PHASES = TICKS + 2

NORM_EPS = 1e-05
CHUNKS = 4


def shifted(value, axis, steps):
    count = lax.axis_size(axis)
    pairs = [(source, (source + steps) % count) for source in range(count)]
    return lax.ppermute(value, axis, pairs)


def moved(value, axis, parity):
    count = lax.axis_size(axis)
    pairs = [((target - 2) % count, target) for target in range(count) if target % 2 == parity]
    return lax.ppermute(value, axis, pairs)


def swapped(value, axis):
    return lax.ppermute(value, axis, [(s, s + 1 - 2 * (s % 2)) for s in range(lax.axis_size(axis))])


def exchange(blocks, axis):
    return lax.all_to_all(blocks, axis, split_axis=0, concat_axis=0, tiled=True)


def head_context(block_of, count, breadth, gain_of, weights_of, normed_ref):
    features = count * breadth
    step = features // CHUNKS
    rows = normed_ref.shape[0]

    def row_sums(values_of):
        total = jnp.zeros((rows, HD), jnp.float32)
        for b in range(count):
            value = values_of(b)
            for c in range(breadth // HD):
                total = total + value[:, c * HD : (c + 1) * HD]
        return jnp.sum(total, axis=-1, keepdims=True)

    mean = row_sums(block_of) * (1.0 / features)

    def squares(b):
        centered = block_of(b) - mean
        return centered * centered

    var = row_sums(squares) * (1.0 / features)
    scale = lax.rsqrt(var + NORM_EPS)
    for b in range(count):
        gain = gain_of(b).astype(jnp.float32)
        normed_ref[:, b * breadth : (b + 1) * breadth] = ((block_of(b) - mean) * scale * gain).astype(
            jnp.bfloat16
        )
    parts = [jnp.zeros((rows, HD), jnp.float32) for _ in range(3)]
    for c in range(CHUNKS):
        piece = normed_ref[:, c * step : (c + 1) * step]
        w_ref = weights_of(c)
        for j in range(3):
            parts[j] = parts[j] + jnp.dot(
                piece, w_ref[j, c * step : (c + 1) * step, :], preferred_element_type=jnp.float32
            )
    queries, keys, values = (part.astype(jnp.bfloat16) for part in parts)
    scores = lax.dot_general(
        queries, keys, (((1,), (1,)), ((), ())), preferred_element_type=jnp.float32
    ) * HD ** (-0.5)
    causal = lax.broadcasted_iota(jnp.int32, scores.shape, 0) >= lax.broadcasted_iota(
        jnp.int32, scores.shape, 1
    )
    scores = jnp.where(causal, scores, -jnp.inf)
    weights = jnp.exp(scores - jnp.max(scores, axis=-1, keepdims=True))
    probs = (weights / jnp.sum(weights, axis=-1, keepdims=True)).astype(jnp.bfloat16)
    return jnp.dot(probs, values, preferred_element_type=jnp.float32).astype(jnp.bfloat16)


def opening_kernel(
    lost_ref, x_hbm, gain_hbm, w_hbm, mix_hbm, out_ref, x_sh_ref, x_ref, gain_ref, normed_ref, w_ref, sems, w_sems, mix_sems
):
    count = out_ref.shape[0]
    rows, features = x_ref.shape
    breadth = features // count
    step = features // CHUNKS
    x_copy = pltpu.make_async_copy(x_hbm, x_ref, sems.at[0])
    gain_copy = pltpu.make_async_copy(gain_hbm, gain_ref, sems.at[1])
    w_copies = [
        pltpu.make_async_copy(
            w_hbm.at[:, pl.ds(c * step, step), :], w_ref.at[:, pl.ds(c * step, step), :], w_sems.at[c]
        )
        for c in range(CHUNKS)
    ]
    mix_copies = [
        pltpu.make_async_copy(
            mix_hbm.at[:, pl.ds(b * breadth, breadth)], out_ref.at[b, :, pl.ds(0, breadth)], mix_sems.at[b]
        )
        for b in range(count)
    ]
    for copy in [x_copy, gain_copy, *w_copies, *mix_copies]:
        copy.start()
    dead = lost_ref[0] == lax.axis_index("section")

    def block_of(b):
        block = x_ref[:, b * breadth : (b + 1) * breadth].astype(jnp.float32)
        return jnp.where(dead, 0.0, block)

    def weights_of(c):
        w_copies[c].wait()
        return w_ref

    def gain_of(b):
        return gain_ref[:, b * breadth : (b + 1) * breadth]

    x_copy.wait()
    gain_copy.wait()
    context = head_context(block_of, count, breadth, gain_of, weights_of, normed_ref)
    for b in range(count):
        out_ref[b, :, breadth:] = context
    start = pl.multiple_of(lax.axis_index("tp") * breadth, breadth)
    x_sh = x_ref[:, pl.ds(start, breadth)]
    x_sh_ref[...] = jnp.where(dead, jnp.zeros_like(x_sh), x_sh)
    for copy in mix_copies:
        copy.wait()


def phase_kernel(x_ref, pack_ref, w_ref, out_ref, normed_ref):
    count, _, breadth = x_ref.shape

    def gain_of(b):
        return pack_ref[count, b : b + 1, :]

    context = head_context(
        lambda b: x_ref[b].astype(jnp.float32), count, breadth, gain_of, lambda c: w_ref, normed_ref
    )
    for b in range(count):
        out_ref[b] = context


def mix_kernel(x_ref, heads_ref, mixed_ref, out_ref):
    branch = jnp.zeros(x_ref.shape, jnp.float32)
    for h in range(heads_ref.shape[0]):
        branch = branch + jnp.dot(heads_ref[h], mixed_ref[h], preferred_element_type=jnp.float32)
    out_ref[...] = (x_ref[...].astype(jnp.float32) + branch).astype(jnp.bfloat16)


def first_mix_kernel(x_ref, joint_ref, gain_ref, out_ref, pack_ref):
    count, breadth = joint_ref.shape[0], x_ref.shape[1]
    branch = jnp.zeros(x_ref.shape, jnp.float32)
    for h in range(count):
        branch = branch + jnp.dot(
            joint_ref[h, :, breadth:], joint_ref[h, :, :breadth], preferred_element_type=jnp.float32
        )
    out_ref[...] = (x_ref[...].astype(jnp.float32) + branch).astype(jnp.bfloat16)
    for h in range(count):
        pack_ref[h] = joint_ref[h, :, :breadth]
    pack_ref[count] = jnp.zeros(x_ref.shape, jnp.bfloat16)
    for b in range(count):
        pack_ref[count, b : b + 1] = gain_ref[:, b * breadth : (b + 1) * breadth]


def lost_near_end(lost, sections):
    return (lost == sections - 2) | (lost == sections - 3)


def enter_kernel(following, lost_ref, plan_ref, moved_ref, stayed_ref, pool_ref, kept_ref, x_ref, copies_ref, keep_ref):
    sections, mine, lost = lax.axis_size("section"), lax.axis_index("section"), lost_ref[0]
    late = lost_near_end(lost, sections)
    phase = following - 1
    rows = jnp.where(mine % 2 == phase % 2, moved_ref[...], stayed_ref[...])
    if keep_ref is not None:
        before = (mine + sections - 1) % sections
        ahead = before - lost
        if phase == 2:
            here = (before != 0) & (ahead == 1)
        else:
            here = jnp.where(before == 0, ~late, (ahead < 1) | (ahead > 3))
        kept = jnp.zeros_like(rows) if kept_ref is None else kept_ref[...]
        keep_ref[...] = jnp.where(here, rows, kept)
    first = mine == (0 if following % 2 == 1 else 1)
    if following == 4:
        first = first & late
    if following == 5:
        first = first & ~late
    rows = jnp.where(first, pool_ref[plan_ref[min(following - 2, TICKS - 1)]], rows)
    if following == 3:
        rows = jnp.where((mine == lost) & (lost == sections - 1), jnp.zeros_like(rows), rows)
    x_ref[...] = rows
    for b in range(copies_ref.shape[0]):
        copies_ref[b] = rows


def later_kernel(lost_ref, fifth_ref, fourth_ref, out_ref):
    sections, mine, lost = lax.axis_size("section"), lax.axis_index("section"), lost_ref[0]
    count, _, breadth = fifth_ref.shape
    behind = mine - lost
    late = lost_near_end(lost, sections)
    second = ((mine == 0) & ~late) | ((mine != 0) & (behind >= 1) & (behind <= 3))

    def store(block_of):
        for b in range(count):
            out_ref[:, b * breadth : (b + 1) * breadth] = block_of(b)

    @pl.when(mine == lost)
    def _():
        store(lambda b: jnp.zeros(fifth_ref.shape[1:], jnp.bfloat16))

    @pl.when((mine != lost) & second)
    def _():
        store(lambda b: fifth_ref[b])

    @pl.when((mine != lost) & ~second)
    def _():
        store(lambda b: fourth_ref[b])


def standby_kernel(lost_ref, arrived_ref, kept_ref, out_ref):
    sections, mine, lost = lax.axis_size("section"), lax.axis_index("section"), lost_ref[0]
    before = (mine + sections - 1) % sections
    ahead = before - lost
    here = ((before == 0) & lost_near_end(lost, sections)) | ((before != 0) & (ahead >= 2) & (ahead <= 3))
    out_ref[...] = jnp.where(here, arrived_ref[...], kept_ref[...])


VMEM = pl.BlockSpec(memory_space=pltpu.VMEM)
SMEM = pl.BlockSpec(memory_space=pltpu.SMEM)
HBM = pl.BlockSpec(memory_space=pltpu.HBM)
LIMIT = pltpu.CompilerParams(vmem_limit_bytes=16 * 1024 * 1024)
WHOLE = pltpu.CompilerParams(vmem_limit_bytes=60 * 1024 * 1024)


def opening(lost, x_full, gain, w_in, mixing, members):
    rows, features = x_full.shape
    breadth = features // members
    return pl.pallas_call(
        opening_kernel,
        out_shape=[
            jax.ShapeDtypeStruct((members, rows, breadth + HD), jnp.bfloat16),
            jax.ShapeDtypeStruct((rows, breadth), jnp.bfloat16),
        ],
        in_specs=[SMEM, HBM, HBM, HBM, HBM],
        out_specs=[VMEM, VMEM],
        scratch_shapes=[
            pltpu.VMEM((rows, features), jnp.bfloat16),
            pltpu.VMEM((1, features), jnp.bfloat16),
            pltpu.VMEM((rows, features), jnp.bfloat16),
            pltpu.VMEM((3, features, HD), jnp.bfloat16),
            pltpu.SemaphoreType.DMA((2,)),
            pltpu.SemaphoreType.DMA((CHUNKS,)),
            pltpu.SemaphoreType.DMA((members,)),
        ],
        compiler_params=WHOLE,
        name="opening",
    )(lost, x_full, gain, w_in, mixing)


def contexts(x_blocks, pack, w_in):
    members, rows, breadth = x_blocks.shape
    return pl.pallas_call(
        phase_kernel,
        out_shape=jax.ShapeDtypeStruct((members, rows, HD), jnp.bfloat16),
        in_specs=[VMEM, VMEM, VMEM],
        out_specs=VMEM,
        scratch_shapes=[pltpu.VMEM((rows, members * breadth), jnp.bfloat16)],
        compiler_params=LIMIT,
        name="contexts",
    )(x_blocks, pack, w_in)


def mixed_rows(x_sh, heads, mixed):
    return pl.pallas_call(
        mix_kernel,
        out_shape=jax.ShapeDtypeStruct(x_sh.shape, jnp.bfloat16),
        in_specs=[VMEM, VMEM, VMEM],
        out_specs=VMEM,
        compiler_params=LIMIT,
        name="mixed_rows",
    )(x_sh, heads, mixed)


def first_mixed_rows(x_sh, joint, gain):
    members, rows, _ = joint.shape
    return pl.pallas_call(
        first_mix_kernel,
        out_shape=[
            jax.ShapeDtypeStruct(x_sh.shape, jnp.bfloat16),
            jax.ShapeDtypeStruct((members + 1, rows, x_sh.shape[1]), jnp.bfloat16),
        ],
        in_specs=[VMEM, VMEM, VMEM],
        out_specs=[VMEM, VMEM],
        compiler_params=LIMIT,
        name="first_mixed_rows",
    )(x_sh, joint, gain)


def entering_rows(following, lost, plan, moved_rows, stayed_rows, pool, kept, members):
    keeps = following % 2 == 1
    operands = [lost, plan, moved_rows, stayed_rows, pool]
    if kept is not None:
        operands.append(kept)
    shape = jax.ShapeDtypeStruct(stayed_rows.shape, jnp.bfloat16)
    copies = jax.ShapeDtypeStruct((members, *stayed_rows.shape), jnp.bfloat16)

    def body(*refs):
        inputs, outputs = list(refs[: len(operands)]), list(refs[len(operands) :])
        if kept is None:
            inputs.append(None)
        if not keeps:
            outputs.append(None)
        enter_kernel(following, *inputs, *outputs)

    return pl.pallas_call(
        body,
        out_shape=[shape, copies] + [shape] * keeps,
        in_specs=[SMEM, SMEM] + [VMEM] * (len(operands) - 2),
        out_specs=[VMEM] * (2 + keeps),
        compiler_params=LIMIT,
        name="entering_rows",
    )(*operands)


def later_rows(lost, fifth, fourth):
    members, rows, breadth = fifth.shape
    return pl.pallas_call(
        later_kernel,
        out_shape=jax.ShapeDtypeStruct((rows, members * breadth), jnp.bfloat16),
        in_specs=[SMEM, VMEM, VMEM],
        out_specs=VMEM,
        compiler_params=LIMIT,
        name="later_rows",
    )(lost, fifth, fourth)


def standby_rows(lost, arrived, kept):
    return pl.pallas_call(
        standby_kernel,
        out_shape=jax.ShapeDtypeStruct(kept.shape, jnp.bfloat16),
        in_specs=[SMEM, VMEM, VMEM],
        out_specs=VMEM,
        compiler_params=LIMIT,
        name="standby_rows",
    )(lost, arrived, kept)


def per_device(
    pending_activation,
    admissible_microbatches,
    arrival_plan,
    vanished_hop,
    query_key_value_matrices,
    mixing_projection_matrices,
    normalizer_factors,
):
    members = lax.axis_size("tp")
    w_in = jnp.moveaxis(query_key_value_matrices[0], 1, 0)
    other_w = swapped(w_in, "section")
    sent, x_sh = opening(
        vanished_hop, pending_activation[0], normalizer_factors, w_in, mixing_projection_matrices[0], members
    )
    y_sh, pack = first_mixed_rows(x_sh, exchange(sent, "tp"), normalizer_factors)
    other_pack = swapped(pack, "section")

    kept = None
    for following in range(2, PHASES + 1):
        moved_rows = moved(y_sh, "section", (following - 1) % 2)
        x_sh, copies, *keep = entering_rows(
            following, vanished_hop, arrival_plan, moved_rows, y_sh, admissible_microbatches, kept, members
        )
        if keep:
            kept = keep[0]
        if following == PHASES:
            copies, fourth = lax.optimization_barrier((copies, fourth))
        x_blocks = exchange(copies, "tp")
        if following == PHASES - 1:
            fourth = swapped(x_blocks, "section")
        layer_w, layer_pack = (w_in, pack) if following % 2 == 1 else (other_w, other_pack)
        heads = exchange(contexts(x_blocks, layer_pack, layer_w), "tp")
        y_sh = mixed_rows(x_sh, heads, layer_pack)
    y_sh, x_blocks, fourth = lax.optimization_barrier((y_sh, x_blocks, fourth))
    arrived = shifted(y_sh, "section", 1)
    later = later_rows(vanished_hop, x_blocks, fourth)
    return (later[None], standby_rows(vanished_hop, arrived, kept)[None])


def solution(mesh):
    placed = (
        P("section", None, None),
        P(None, None, "tp"),
        P(),
        P(),
        P("section", None, None, "tp"),
        P("section", "tp", None),
        P("section", None),
    )
    return jax.shard_map(
        per_device,
        mesh=mesh,
        in_specs=placed,
        out_specs=(P("section", None, None), P("section", None, "tp")),
        check_vma=False,
    )
```

```python
import functools

import jax
import jax.numpy as jnp
from jax import lax
from jax.experimental import pallas as pl
from jax.experimental.pallas import tpu as pltpu
from jax.sharding import PartitionSpec as P

HD = 128
TICKS = 3
PHASES = TICKS + 2

NORM_EPS = 1e-05
CHUNKS = 4
MOVES = {1: (1, 2), 3: (1, 2), 4: (0, 4)}


def shifted(value, axis, steps):
    count = lax.axis_size(axis)
    pairs = [(source, (source + steps) % count) for source in range(count)]
    return lax.ppermute(value, axis, pairs)


def moved(value, axis, parity, steps):
    count = lax.axis_size(axis)
    pairs = [((target - steps) % count, target) for target in range(count) if target % 2 == parity]
    return lax.ppermute(value, axis, pairs)


def swapped(value, axis):
    return lax.ppermute(value, axis, [(s, s + 1 - 2 * (s % 2)) for s in range(lax.axis_size(axis))])


def home_of_fourth(value, axis):
    count = lax.axis_size(axis)
    return lax.ppermute(value, axis, [(s, (s + 3) % count if s % 2 == 0 else s - 1) for s in range(count)])


def exchange(blocks, axis):
    return lax.all_to_all(blocks, axis, split_axis=0, concat_axis=0, tiled=True)


def head_context(block_of, count, breadth, gain_of, weights_of, normed_ref):
    features = count * breadth
    step = features // CHUNKS
    rows = normed_ref.shape[0]

    def row_sums(values_of):
        total = jnp.zeros((rows, HD), jnp.float32)
        for b in range(count):
            value = values_of(b)
            for c in range(breadth // HD):
                total = total + value[:, c * HD : (c + 1) * HD]
        return jnp.sum(total, axis=-1, keepdims=True)

    mean = row_sums(block_of) * (1.0 / features)

    def squares(b):
        centered = block_of(b) - mean
        return centered * centered

    var = row_sums(squares) * (1.0 / features)
    scale = lax.rsqrt(var + NORM_EPS)
    for b in range(count):
        gain = gain_of(b).astype(jnp.float32)
        normed_ref[:, b * breadth : (b + 1) * breadth] = ((block_of(b) - mean) * scale * gain).astype(
            jnp.bfloat16
        )
    parts = [jnp.zeros((rows, HD), jnp.float32) for _ in range(3)]
    for c in range(CHUNKS):
        piece = normed_ref[:, c * step : (c + 1) * step]
        w_ref = weights_of(c)
        for j in range(3):
            parts[j] = parts[j] + jnp.dot(
                piece, w_ref[j, c * step : (c + 1) * step, :], preferred_element_type=jnp.float32
            )
    queries, keys, values = (part.astype(jnp.bfloat16) for part in parts)
    scores = lax.dot_general(
        queries, keys, (((1,), (1,)), ((), ())), preferred_element_type=jnp.float32
    ) * HD ** (-0.5)
    causal = lax.broadcasted_iota(jnp.int32, scores.shape, 0) >= lax.broadcasted_iota(
        jnp.int32, scores.shape, 1
    )
    scores = jnp.where(causal, scores, -jnp.inf)
    weights = jnp.exp(scores - jnp.max(scores, axis=-1, keepdims=True))
    probs = (weights / jnp.sum(weights, axis=-1, keepdims=True)).astype(jnp.bfloat16)
    return jnp.dot(probs, values, preferred_element_type=jnp.float32).astype(jnp.bfloat16)


def opening_kernel(
    lost_ref, x_hbm, gain_hbm, w_hbm, mix_hbm, out_ref, x_sh_ref, x_ref, gain_ref, normed_ref, w_ref, sems, w_sems, mix_sems
):
    count = out_ref.shape[0]
    _, features = x_ref.shape
    breadth = features // count
    step = features // CHUNKS
    x_copy = pltpu.make_async_copy(x_hbm, x_ref, sems.at[0])
    gain_copy = pltpu.make_async_copy(gain_hbm, gain_ref, sems.at[1])
    w_copies = [
        pltpu.make_async_copy(
            w_hbm.at[:, pl.ds(c * step, step), :], w_ref.at[:, pl.ds(c * step, step), :], w_sems.at[c]
        )
        for c in range(CHUNKS)
    ]
    mix_copies = [
        pltpu.make_async_copy(
            mix_hbm.at[:, pl.ds(b * breadth, breadth)], out_ref.at[b, :, pl.ds(0, breadth)], mix_sems.at[b]
        )
        for b in range(count)
    ]
    for copy in [x_copy, gain_copy, *w_copies, *mix_copies]:
        copy.start()
    dead = lost_ref[0] == lax.axis_index("section")

    def block_of(b):
        block = x_ref[:, b * breadth : (b + 1) * breadth].astype(jnp.float32)
        return jnp.where(dead, 0.0, block)

    def weights_of(c):
        w_copies[c].wait()
        return w_ref

    def gain_of(b):
        return gain_ref[:, b * breadth : (b + 1) * breadth]

    x_copy.wait()
    gain_copy.wait()
    context = head_context(block_of, count, breadth, gain_of, weights_of, normed_ref)
    for b in range(count):
        out_ref[b, :, breadth:] = context
    start = pl.multiple_of(lax.axis_index("tp") * breadth, breadth)
    x_sh = x_ref[:, pl.ds(start, breadth)]
    x_sh_ref[...] = jnp.where(dead, jnp.zeros_like(x_sh), x_sh)
    for copy in mix_copies:
        copy.wait()


def by_parity(*bodies):
    if len(bodies) == 1:
        bodies[0]()
        return
    for parity, body in enumerate(bodies):
        pl.when(lax.axis_index("section") % 2 == parity)(body)


def phase_kernel(x_ref, *refs):
    *layers, out_ref, normed_ref = refs
    count, _, breadth = x_ref.shape

    def body(pack_ref, w_ref):
        context = head_context(
            lambda b: x_ref[b].astype(jnp.float32),
            count,
            breadth,
            lambda b: pack_ref[count, b : b + 1, :],
            lambda c: w_ref,
            normed_ref,
        )
        for b in range(count):
            out_ref[b] = context

    by_parity(*(functools.partial(body, *layers[i : i + 2]) for i in range(0, len(layers), 2)))


def mix_kernel(x_ref, heads_ref, *refs):
    *packs, out_ref = refs

    def body(pack_ref):
        branch = jnp.zeros(x_ref.shape, jnp.float32)
        for h in range(heads_ref.shape[0]):
            branch = branch + jnp.dot(heads_ref[h], pack_ref[h], preferred_element_type=jnp.float32)
        out_ref[...] = (x_ref[...].astype(jnp.float32) + branch).astype(jnp.bfloat16)

    by_parity(*(functools.partial(body, pack) for pack in packs))


def first_mix_kernel(x_ref, joint_ref, gain_ref, out_ref, pack_ref):
    count, breadth = joint_ref.shape[0], x_ref.shape[1]
    branch = jnp.zeros(x_ref.shape, jnp.float32)
    for h in range(count):
        branch = branch + jnp.dot(
            joint_ref[h, :, breadth:], joint_ref[h, :, :breadth], preferred_element_type=jnp.float32
        )
    out_ref[...] = (x_ref[...].astype(jnp.float32) + branch).astype(jnp.bfloat16)
    for h in range(count):
        pack_ref[h] = joint_ref[h, :, :breadth]
    pack_ref[count] = jnp.zeros(x_ref.shape, jnp.bfloat16)
    for b in range(count):
        pack_ref[count, b : b + 1] = gain_ref[:, b * breadth : (b + 1) * breadth]


def lost_near_end(lost, sections):
    return (lost == sections - 2) | (lost == sections - 3)


def role(phase, mine, sections):
    even = {1: 0, 2: 1, 3: 2, 4: 3, 5: 0}[phase]
    odd = {1: 0, 2: -1, 3: 0, 4: -1, 5: 0}[phase]
    return (mine + sections + jnp.where(mine % 2 == 0, even, odd)) % sections


def enter_kernel(following, refs):
    sections, mine, lost = lax.axis_size("section"), lax.axis_index("section"), refs["lost"][0]
    here_for = role(following, mine, sections)
    late = lost_near_end(lost, sections)
    phase = following - 1
    rows = refs["stayed"][...]
    if "moved" in refs:
        rows = jnp.where(mine % 2 == MOVES[phase][0], refs["moved"][...], rows)
    if "keep" in refs:
        before = (here_for + sections - 1) % sections
        ahead = before - lost
        if phase == 2:
            here = (before != 0) & (ahead == 1)
            kept = jnp.zeros_like(rows)
        else:
            here = jnp.where(before == 0, ~late, (ahead < 1) | (ahead > 3))
            kept = jnp.where(mine % 2 == 0, refs["kept_even"][...], refs["kept_odd"][...])
        refs["keep"][...] = jnp.where(here, rows, kept)
    first = here_for == 0
    if following == 4:
        first = first & late
    if following == 5:
        first = first & ~late
    rows = jnp.where(first, refs["pool"][refs["plan"][min(following - 2, TICKS - 1)]], rows)
    if following == 3:
        rows = jnp.where((here_for == lost) & (lost == sections - 1), jnp.zeros_like(rows), rows)
    refs["x"][...] = rows
    for b in range(refs["copies"].shape[0]):
        refs["copies"][b] = rows


def later_kernel(lost_ref, fifth_ref, fourth_ref, out_ref):
    sections, mine, lost = lax.axis_size("section"), lax.axis_index("section"), lost_ref[0]
    count, _, breadth = fifth_ref.shape
    behind = mine - lost
    late = lost_near_end(lost, sections)
    second = ((mine == 0) & ~late) | ((mine != 0) & (behind >= 1) & (behind <= 3))

    def store(block_of):
        for b in range(count):
            out_ref[:, b * breadth : (b + 1) * breadth] = block_of(b)

    @pl.when(mine == lost)
    def _():
        store(lambda b: jnp.zeros(fifth_ref.shape[1:], jnp.bfloat16))

    @pl.when((mine != lost) & second)
    def _():
        store(lambda b: fifth_ref[b])

    @pl.when((mine != lost) & ~second)
    def _():
        store(lambda b: fourth_ref[b])


def standby_kernel(lost_ref, arrived_ref, kept_ref, out_ref):
    sections, mine, lost = lax.axis_size("section"), lax.axis_index("section"), lost_ref[0]
    before = (mine + sections - 1) % sections
    ahead = before - lost
    here = ((before == 0) & lost_near_end(lost, sections)) | ((before != 0) & (ahead >= 2) & (ahead <= 3))
    out_ref[...] = jnp.where(here, arrived_ref[...], kept_ref[...])


VMEM = pl.BlockSpec(memory_space=pltpu.VMEM)
SMEM = pl.BlockSpec(memory_space=pltpu.SMEM)
HBM = pl.BlockSpec(memory_space=pltpu.HBM)
LIMIT = pltpu.CompilerParams(vmem_limit_bytes=16 * 1024 * 1024)
WHOLE = pltpu.CompilerParams(vmem_limit_bytes=57 * 1024 * 1024)


def opening(lost, x_full, gain, w_in, mixing, members):
    rows, features = x_full.shape
    breadth = features // members
    return pl.pallas_call(
        opening_kernel,
        out_shape=[
            jax.ShapeDtypeStruct((members, rows, breadth + HD), jnp.bfloat16),
            jax.ShapeDtypeStruct((rows, breadth), jnp.bfloat16),
        ],
        in_specs=[SMEM, HBM, HBM, HBM, HBM],
        out_specs=[VMEM, VMEM],
        scratch_shapes=[
            pltpu.VMEM((rows, features), jnp.bfloat16),
            pltpu.VMEM((1, features), jnp.bfloat16),
            pltpu.VMEM((rows, features), jnp.bfloat16),
            pltpu.VMEM((3, features, HD), jnp.bfloat16),
            pltpu.SemaphoreType.DMA((2,)),
            pltpu.SemaphoreType.DMA((CHUNKS,)),
            pltpu.SemaphoreType.DMA((members,)),
        ],
        compiler_params=WHOLE,
        name="opening",
    )(lost, x_full, gain, w_in, mixing)


def contexts(x_blocks, layers):
    members, rows, breadth = x_blocks.shape
    operands = [x_blocks, *(array for layer in layers for array in layer)]
    return pl.pallas_call(
        phase_kernel,
        out_shape=jax.ShapeDtypeStruct((members, rows, HD), jnp.bfloat16),
        in_specs=[VMEM] * len(operands),
        out_specs=VMEM,
        scratch_shapes=[pltpu.VMEM((rows, members * breadth), jnp.bfloat16)],
        compiler_params=LIMIT,
        name="contexts",
    )(*operands)


def mixed_rows(x_sh, heads, packs):
    return pl.pallas_call(
        mix_kernel,
        out_shape=jax.ShapeDtypeStruct(x_sh.shape, jnp.bfloat16),
        in_specs=[VMEM] * (2 + len(packs)),
        out_specs=VMEM,
        compiler_params=LIMIT,
        name="mixed_rows",
    )(x_sh, heads, *packs)


def first_mixed_rows(x_sh, joint, gain):
    members, rows, _ = joint.shape
    return pl.pallas_call(
        first_mix_kernel,
        out_shape=[
            jax.ShapeDtypeStruct(x_sh.shape, jnp.bfloat16),
            jax.ShapeDtypeStruct((members + 1, rows, x_sh.shape[1]), jnp.bfloat16),
        ],
        in_specs=[VMEM, VMEM, VMEM],
        out_specs=[VMEM, VMEM],
        compiler_params=LIMIT,
        name="first_mixed_rows",
    )(x_sh, joint, gain)


def entering_rows(following, members, **operands):
    names = list(operands)
    rows = jax.ShapeDtypeStruct(operands["stayed"].shape, jnp.bfloat16)
    outs = {"x": rows, "copies": jax.ShapeDtypeStruct((members, *rows.shape), jnp.bfloat16)}
    if following % 2 == 1:
        outs["keep"] = rows

    def body(*refs):
        enter_kernel(following, dict(zip([*names, *outs], refs, strict=True)))

    results = pl.pallas_call(
        body,
        out_shape=list(outs.values()),
        in_specs=[SMEM if name in ("lost", "plan") else VMEM for name in names],
        out_specs=[VMEM] * len(outs),
        compiler_params=LIMIT,
        name="entering_rows",
    )(*operands.values())
    return dict(zip(outs, results, strict=True))


def later_rows(lost, fifth, fourth):
    members, rows, breadth = fifth.shape
    return pl.pallas_call(
        later_kernel,
        out_shape=jax.ShapeDtypeStruct((rows, members * breadth), jnp.bfloat16),
        in_specs=[SMEM, VMEM, VMEM],
        out_specs=VMEM,
        compiler_params=LIMIT,
        name="later_rows",
    )(lost, fifth, fourth)


def standby_rows(lost, arrived, kept):
    return pl.pallas_call(
        standby_kernel,
        out_shape=jax.ShapeDtypeStruct(kept.shape, jnp.bfloat16),
        in_specs=[SMEM, VMEM, VMEM],
        out_specs=VMEM,
        compiler_params=LIMIT,
        name="standby_rows",
    )(lost, arrived, kept)


def per_device(
    pending_activation,
    admissible_microbatches,
    arrival_plan,
    vanished_hop,
    query_key_value_matrices,
    mixing_projection_matrices,
    normalizer_factors,
):
    members = lax.axis_size("tp")
    w_in = jnp.moveaxis(query_key_value_matrices[0], 1, 0)
    other_w = swapped(w_in, "section")
    next_w = moved(w_in, "section", 0, -2)
    sent, x_sh = opening(
        vanished_hop, pending_activation[0], normalizer_factors, w_in, mixing_projection_matrices[0], members
    )
    y_sh, pack = first_mixed_rows(x_sh, exchange(sent, "tp"), normalizer_factors)
    other_pack = swapped(pack, "section")
    next_pack = moved(pack, "section", 0, -2)
    pack, far_w = lax.optimization_barrier((pack, other_w))
    far_w = moved(far_w, "section", 0, -2)

    kept = {}
    for following in range(2, PHASES + 1):
        phase = following - 1
        if phase in MOVES:
            kept["moved"] = moved(y_sh, "section", *MOVES[phase])
        rows = entering_rows(
            following,
            members,
            lost=vanished_hop,
            plan=arrival_plan,
            stayed=y_sh,
            pool=admissible_microbatches,
            **kept,
        )
        kept = {}
        copies = rows["copies"]
        if following == 2:
            copies, other_pack = lax.optimization_barrier((copies, other_pack))
        if following == 3:
            copies, next_w, next_pack = lax.optimization_barrier((copies, next_w, next_pack))
        if following == 4:
            copies, far_w, far_pack = lax.optimization_barrier((copies, far_w, far_pack))
        if following == PHASES:
            copies, fourth = lax.optimization_barrier((copies, fourth))
        x_blocks = exchange(copies, "tp")
        if following == PHASES - 1:
            fourth = home_of_fourth(x_blocks, "section")
        layers = {
            2: lambda: [(other_pack, other_w)],
            3: lambda: [(next_pack, next_w), (pack, w_in)],
            4: lambda: [(far_pack, far_w), (other_pack, other_w)],
            5: lambda: [(pack, w_in)],
        }[following]()
        heads = exchange(contexts(x_blocks, layers), "tp")
        y_sh = mixed_rows(rows["x"], heads, [layer[0] for layer in layers])
        if following == 2:
            y_sh, far_pack = lax.optimization_barrier((y_sh, other_pack))
            far_pack = moved(far_pack, "section", 0, -2)
        if following == 3:
            kept_second = rows["keep"]
        if following == 3:
            y_sh, kept_second = lax.optimization_barrier((y_sh, kept_second))
            kept = {"kept_odd": kept_second, "kept_even": moved(kept_second, "section", 0, 2)}
            kept_for_last = kept
            kept = {}
        if following == 4:
            kept = kept_for_last
    y_sh, x_blocks, fourth = lax.optimization_barrier((y_sh, x_blocks, fourth))
    arrived = shifted(y_sh, "section", 1)
    later = later_rows(vanished_hop, x_blocks, fourth)
    return (later[None], standby_rows(vanished_hop, arrived, rows["keep"])[None])


def solution(mesh):
    placed = (
        P("section", None, None),
        P(None, None, "tp"),
        P(),
        P(),
        P("section", None, None, "tp"),
        P("section", "tp", None),
        P("section", None),
    )


    return jax.shard_map(
        per_device,
        mesh=mesh,
        in_specs=placed,
        out_specs=(P("section", None, None), P("section", None, "tp")),
        check_vma=False,
    )
```

```python
import jax
import jax.numpy as jnp
from jax import lax
from jax.experimental import pallas as pl
from jax.experimental.pallas import tpu as pltpu
from jax.sharding import PartitionSpec as P

HD = 128
TICKS = 3
PHASES = TICKS + 2

NORM_EPS = 1e-05
CHUNKS = 4


def shifted(value, axis, steps):
    count = lax.axis_size(axis)
    pairs = [(source, (source + steps) % count) for source in range(count)]
    return lax.ppermute(value, axis, pairs)


def moved(value, axis, parity):
    count = lax.axis_size(axis)
    pairs = [((target - 2) % count, target) for target in range(count) if target % 2 == parity]
    return lax.ppermute(value, axis, pairs)


def swapped(value, axis):
    return lax.ppermute(value, axis, [(s, s + 1 - 2 * (s % 2)) for s in range(lax.axis_size(axis))])


def exchange(blocks, axis):
    return lax.all_to_all(blocks, axis, split_axis=0, concat_axis=0, tiled=True)


def head_context(block_of, count, breadth, gain_of, weights_of, normed_ref):
    features = count * breadth
    step = features // CHUNKS
    rows = normed_ref.shape[0]

    def row_sums(values_of):
        total = jnp.zeros((rows, HD), jnp.float32)
        for b in range(count):
            value = values_of(b)
            for c in range(breadth // HD):
                total = total + value[:, c * HD : (c + 1) * HD]
        return jnp.sum(total, axis=-1, keepdims=True)

    mean = row_sums(block_of) * (1.0 / features)

    def squares(b):
        centered = block_of(b) - mean
        return centered * centered

    var = row_sums(squares) * (1.0 / features)
    scale = lax.rsqrt(var + NORM_EPS)
    for b in range(count):
        gain = gain_of(b).astype(jnp.float32)
        normed_ref[:, b * breadth : (b + 1) * breadth] = ((block_of(b) - mean) * scale * gain).astype(
            jnp.bfloat16
        )
    projected = jnp.zeros((rows, 3 * HD), jnp.float32)
    for c in range(CHUNKS):
        w_ref = weights_of(c)
        side_by_side = jnp.concatenate([w_ref[j, c * step : (c + 1) * step, :] for j in range(3)], axis=1)
        projected = projected + jnp.dot(
            normed_ref[:, c * step : (c + 1) * step], side_by_side, preferred_element_type=jnp.float32
        )
    projected = projected.astype(jnp.bfloat16)
    queries, keys, values = projected[:, :HD], projected[:, HD : 2 * HD], projected[:, 2 * HD :]
    scores = lax.dot_general(
        queries, keys, (((1,), (1,)), ((), ())), preferred_element_type=jnp.float32
    ) * HD ** (-0.5)
    causal = lax.broadcasted_iota(jnp.int32, scores.shape, 0) >= lax.broadcasted_iota(
        jnp.int32, scores.shape, 1
    )
    scores = jnp.where(causal, scores, -jnp.inf)
    weights = jnp.exp(scores - jnp.max(scores, axis=-1, keepdims=True))
    probs = (weights / jnp.sum(weights, axis=-1, keepdims=True)).astype(jnp.bfloat16)
    return jnp.dot(probs, values, preferred_element_type=jnp.float32).astype(jnp.bfloat16)


def opening_kernel(
    lost_ref, x_hbm, gain_hbm, w_hbm, mix_hbm, out_ref, x_sh_ref, x_ref, gain_ref, normed_ref, w_ref, sems, x_sems, w_sems, mix_sems
):
    count = out_ref.shape[0]
    rows, features = x_ref.shape
    breadth = features // count
    step = features // CHUNKS
    x_copies = [
        pltpu.make_async_copy(
            x_hbm.at[:, pl.ds(c * step, step)], x_ref.at[:, pl.ds(c * step, step)], x_sems.at[c]
        )
        for c in range(CHUNKS)
    ]
    gain_copy = pltpu.make_async_copy(gain_hbm, gain_ref, sems.at[0])
    w_copies = [
        pltpu.make_async_copy(
            w_hbm.at[:, pl.ds(c * step, step), :], w_ref.at[:, pl.ds(c * step, step), :], w_sems.at[c]
        )
        for c in range(CHUNKS)
    ]
    mix_copies = [
        pltpu.make_async_copy(
            mix_hbm.at[:, pl.ds(b * breadth, breadth)], out_ref.at[b, :, pl.ds(0, breadth)], mix_sems.at[b]
        )
        for b in range(count)
    ]
    for copy in [*x_copies, gain_copy, *w_copies, *mix_copies]:
        copy.start()
    dead = lost_ref[0] == lax.axis_index("section")

    def block_of(b):
        block = x_ref[:, b * breadth : (b + 1) * breadth].astype(jnp.float32)
        return jnp.where(dead, 0.0, block)

    def weights_of(c):
        w_copies[c].wait()
        return w_ref

    def gain_of(b):
        return gain_ref[:, b * breadth : (b + 1) * breadth]

    for copy in [*x_copies, gain_copy]:
        copy.wait()
    context = head_context(block_of, count, breadth, gain_of, weights_of, normed_ref)
    for b in range(count):
        out_ref[b, :, breadth:] = context
    start = pl.multiple_of(lax.axis_index("tp") * breadth, breadth)
    x_sh = x_ref[:, pl.ds(start, breadth)]
    x_sh_ref[...] = jnp.where(dead, jnp.zeros_like(x_sh), x_sh)
    for copy in mix_copies:
        copy.wait()


def phase_kernel(x_ref, pack_ref, w_ref, out_ref, normed_ref):
    count, _, breadth = x_ref.shape

    def gain_of(b):
        return pack_ref[count, b : b + 1, :]

    context = head_context(
        lambda b: x_ref[b].astype(jnp.float32), count, breadth, gain_of, lambda c: w_ref, normed_ref
    )
    for b in range(count):
        out_ref[b] = context


def mix_kernel(x_ref, heads_ref, mixed_ref, out_ref):
    branch = jnp.zeros(x_ref.shape, jnp.float32)
    for h in range(heads_ref.shape[0]):
        branch = branch + jnp.dot(heads_ref[h], mixed_ref[h], preferred_element_type=jnp.float32)
    out_ref[...] = (x_ref[...].astype(jnp.float32) + branch).astype(jnp.bfloat16)


def first_mix_kernel(x_ref, joint_ref, gain_ref, out_ref, pack_ref):
    count, breadth = joint_ref.shape[0], x_ref.shape[1]
    branch = jnp.zeros(x_ref.shape, jnp.float32)
    for h in range(count):
        branch = branch + jnp.dot(
            joint_ref[h, :, breadth:], joint_ref[h, :, :breadth], preferred_element_type=jnp.float32
        )
    out_ref[...] = (x_ref[...].astype(jnp.float32) + branch).astype(jnp.bfloat16)
    for h in range(count):
        pack_ref[h] = joint_ref[h, :, :breadth]
    pack_ref[count] = jnp.zeros(x_ref.shape, jnp.bfloat16)
    for b in range(count):
        pack_ref[count, b : b + 1] = gain_ref[:, b * breadth : (b + 1) * breadth]


def lost_near_end(lost, sections):
    return (lost == sections - 2) | (lost == sections - 3)


def enter_kernel(following, lost_ref, plan_ref, moved_ref, stayed_ref, pool_ref, kept_ref, x_ref, copies_ref, keep_ref):
    sections, mine, lost = lax.axis_size("section"), lax.axis_index("section"), lost_ref[0]
    late = lost_near_end(lost, sections)
    phase = following - 1
    rows = jnp.where(mine % 2 == phase % 2, moved_ref[...], stayed_ref[...])
    if keep_ref is not None:
        before = (mine + sections - 1) % sections
        ahead = before - lost
        if phase == 2:
            here = (before != 0) & (ahead == 1)
        else:
            here = jnp.where(before == 0, ~late, (ahead < 1) | (ahead > 3))
        kept = jnp.zeros_like(rows) if kept_ref is None else kept_ref[...]
        keep_ref[...] = jnp.where(here, rows, kept)
    first = mine == (0 if following % 2 == 1 else 1)
    if following == 4:
        first = first & late
    if following == 5:
        first = first & ~late
    rows = jnp.where(first, pool_ref[plan_ref[min(following - 2, TICKS - 1)]], rows)
    if following == 3:
        rows = jnp.where((mine == lost) & (lost == sections - 1), jnp.zeros_like(rows), rows)
    x_ref[...] = rows
    for b in range(copies_ref.shape[0]):
        copies_ref[b] = rows


def later_kernel(lost_ref, fifth_ref, fourth_ref, out_ref):
    sections, mine, lost = lax.axis_size("section"), lax.axis_index("section"), lost_ref[0]
    count, _, breadth = fifth_ref.shape
    behind = mine - lost
    late = lost_near_end(lost, sections)
    second = ((mine == 0) & ~late) | ((mine != 0) & (behind >= 1) & (behind <= 3))

    def store(block_of):
        for b in range(count):
            out_ref[:, b * breadth : (b + 1) * breadth] = block_of(b)

    @pl.when(mine == lost)
    def _():
        store(lambda b: jnp.zeros(fifth_ref.shape[1:], jnp.bfloat16))

    @pl.when((mine != lost) & second)
    def _():
        store(lambda b: fifth_ref[b])

    @pl.when((mine != lost) & ~second)
    def _():
        store(lambda b: fourth_ref[b])


def standby_kernel(lost_ref, arrived_ref, kept_ref, out_ref):
    sections, mine, lost = lax.axis_size("section"), lax.axis_index("section"), lost_ref[0]
    before = (mine + sections - 1) % sections
    ahead = before - lost
    here = ((before == 0) & lost_near_end(lost, sections)) | ((before != 0) & (ahead >= 2) & (ahead <= 3))
    out_ref[...] = jnp.where(here, arrived_ref[...], kept_ref[...])


VMEM = pl.BlockSpec(memory_space=pltpu.VMEM)
SMEM = pl.BlockSpec(memory_space=pltpu.SMEM)
HBM = pl.BlockSpec(memory_space=pltpu.HBM)
LIMIT = pltpu.CompilerParams(vmem_limit_bytes=16 * 1024 * 1024)
WHOLE = pltpu.CompilerParams(vmem_limit_bytes=57 * 1024 * 1024)


def opening(lost, x_full, gain, w_in, mixing, members):
    rows, features = x_full.shape
    breadth = features // members
    return pl.pallas_call(
        opening_kernel,
        out_shape=[
            pltpu.VMEM((members, rows, breadth + HD), jnp.bfloat16),
            pltpu.VMEM((rows, breadth), jnp.bfloat16),
        ],
        in_specs=[SMEM, HBM, HBM, HBM, HBM],
        out_specs=[VMEM, VMEM],
        scratch_shapes=[
            pltpu.VMEM((rows, features), jnp.bfloat16),
            pltpu.VMEM((1, features), jnp.bfloat16),
            pltpu.VMEM((rows, features), jnp.bfloat16),
            pltpu.VMEM((3, features, HD), jnp.bfloat16),
            pltpu.SemaphoreType.DMA((1,)),
            pltpu.SemaphoreType.DMA((CHUNKS,)),
            pltpu.SemaphoreType.DMA((CHUNKS,)),
            pltpu.SemaphoreType.DMA((members,)),
        ],
        compiler_params=WHOLE,
        name="opening",
    )(lost, x_full, gain, w_in, mixing)


def contexts(x_blocks, pack, w_in):
    members, rows, breadth = x_blocks.shape
    return pl.pallas_call(
        phase_kernel,
        out_shape=jax.ShapeDtypeStruct((members, rows, HD), jnp.bfloat16),
        in_specs=[VMEM, VMEM, VMEM],
        out_specs=VMEM,
        scratch_shapes=[pltpu.VMEM((rows, members * breadth), jnp.bfloat16)],
        compiler_params=LIMIT,
        name="contexts",
    )(x_blocks, pack, w_in)


def mixed_rows(x_sh, heads, mixed):
    return pl.pallas_call(
        mix_kernel,
        out_shape=jax.ShapeDtypeStruct(x_sh.shape, jnp.bfloat16),
        in_specs=[VMEM, VMEM, VMEM],
        out_specs=VMEM,
        compiler_params=LIMIT,
        name="mixed_rows",
    )(x_sh, heads, mixed)


def first_mixed_rows(x_sh, joint, gain):
    members, rows, _ = joint.shape
    return pl.pallas_call(
        first_mix_kernel,
        out_shape=[
            jax.ShapeDtypeStruct(x_sh.shape, jnp.bfloat16),
            jax.ShapeDtypeStruct((members + 1, rows, x_sh.shape[1]), jnp.bfloat16),
        ],
        in_specs=[VMEM, VMEM, VMEM],
        out_specs=[VMEM, VMEM],
        compiler_params=LIMIT,
        name="first_mixed_rows",
    )(x_sh, joint, gain)


def entering_rows(following, lost, plan, moved_rows, stayed_rows, pool, kept, members):
    keeps = following % 2 == 1
    operands = [lost, plan, moved_rows, stayed_rows, pool]
    if kept is not None:
        operands.append(kept)
    shape = jax.ShapeDtypeStruct(stayed_rows.shape, jnp.bfloat16)
    copies = jax.ShapeDtypeStruct((members, *stayed_rows.shape), jnp.bfloat16)

    def body(*refs):
        inputs, outputs = list(refs[: len(operands)]), list(refs[len(operands) :])
        if kept is None:
            inputs.append(None)
        if not keeps:
            outputs.append(None)
        enter_kernel(following, *inputs, *outputs)

    return pl.pallas_call(
        body,
        out_shape=[shape, copies] + [shape] * keeps,
        in_specs=[SMEM, SMEM] + [VMEM] * (len(operands) - 2),
        out_specs=[VMEM] * (2 + keeps),
        compiler_params=LIMIT,
        name="entering_rows",
    )(*operands)


def later_rows(lost, fifth, fourth):
    members, rows, breadth = fifth.shape
    return pl.pallas_call(
        later_kernel,
        out_shape=jax.ShapeDtypeStruct((rows, members * breadth), jnp.bfloat16),
        in_specs=[SMEM, VMEM, VMEM],
        out_specs=VMEM,
        compiler_params=LIMIT,
        name="later_rows",
    )(lost, fifth, fourth)


def standby_rows(lost, arrived, kept):
    return pl.pallas_call(
        standby_kernel,
        out_shape=jax.ShapeDtypeStruct(kept.shape, jnp.bfloat16),
        in_specs=[SMEM, VMEM, VMEM],
        out_specs=VMEM,
        compiler_params=LIMIT,
        name="standby_rows",
    )(lost, arrived, kept)


def per_device(
    pending_activation,
    admissible_microbatches,
    arrival_plan,
    vanished_hop,
    query_key_value_matrices,
    mixing_projection_matrices,
    normalizer_factors,
):
    members = lax.axis_size("tp")
    w_in = jnp.moveaxis(query_key_value_matrices[0], 1, 0)
    other_w = swapped(w_in, "section")
    sent, x_sh = opening(
        vanished_hop, pending_activation[0], normalizer_factors, w_in, mixing_projection_matrices[0], members
    )
    y_sh, pack = first_mixed_rows(x_sh, exchange(sent, "tp"), normalizer_factors)
    other_pack = swapped(pack, "section")

    kept = None
    for following in range(2, PHASES + 1):
        moved_rows = moved(y_sh, "section", (following - 1) % 2)
        x_sh, copies, *keep = entering_rows(
            following, vanished_hop, arrival_plan, moved_rows, y_sh, admissible_microbatches, kept, members
        )
        if keep:
            kept = keep[0]
        if following == PHASES:
            copies, fourth = lax.optimization_barrier((copies, fourth))
        x_blocks = exchange(copies, "tp")
        if following == PHASES - 1:
            fourth = swapped(x_blocks, "section")
        layer_w, layer_pack = (w_in, pack) if following % 2 == 1 else (other_w, other_pack)
        heads = exchange(contexts(x_blocks, layer_pack, layer_w), "tp")
        y_sh = mixed_rows(x_sh, heads, layer_pack)
    y_sh, x_blocks, fourth = lax.optimization_barrier((y_sh, x_blocks, fourth))
    arrived = shifted(y_sh, "section", 1)
    later = later_rows(vanished_hop, x_blocks, fourth)
    return (later[None], standby_rows(vanished_hop, arrived, kept)[None])


def solution(mesh):
    placed = (
        P("section", None, None),
        P(None, None, "tp"),
        P(),
        P(),
        P("section", None, None, "tp"),
        P("section", "tp", None),
        P("section", None),
    )
    return jax.shard_map(
        per_device,
        mesh=mesh,
        in_specs=placed,
        out_specs=(P("section", None, None), P("section", None, "tp")),
        check_vma=False,
    )
```

```python
import jax
import jax.numpy as jnp
from jax import lax
from jax.experimental import pallas as pl
from jax.experimental.pallas import tpu as pltpu
from jax.sharding import PartitionSpec as P

HD = 128
TICKS = 3
PHASES = TICKS + 2

NORM_EPS = 1e-05
CHUNKS = 4


def shifted(value, axis, steps):
    count = lax.axis_size(axis)
    pairs = [(source, (source + steps) % count) for source in range(count)]
    return lax.ppermute(value, axis, pairs)


def moved(value, axis, parity, drop=False):
    count = lax.axis_size(axis)
    pairs = [((target - 2) % count, target) for target in range(count) if target % 2 == parity]
    if drop:
        pairs = [pair for pair in pairs if pair[1] != 1]
    return lax.ppermute(value, axis, pairs)


def swapped(value, axis):
    return lax.ppermute(value, axis, [(s, s + 1 - 2 * (s % 2)) for s in range(lax.axis_size(axis))])


def exchange(blocks, axis):
    return lax.all_to_all(blocks, axis, split_axis=0, concat_axis=0, tiled=True)


def head_context(block_of, count, breadth, gain_of, weights_of, normed_ref):
    features = count * breadth
    step = features // CHUNKS
    rows = normed_ref.shape[0]

    def row_sums(values_of):
        total = jnp.zeros((rows, HD), jnp.float32)
        for b in range(count):
            value = values_of(b)
            for c in range(breadth // HD):
                total = total + value[:, c * HD : (c + 1) * HD]
        return jnp.sum(total, axis=-1, keepdims=True)

    mean = row_sums(block_of) * (1.0 / features)

    def squares(b):
        centered = block_of(b) - mean
        return centered * centered

    var = row_sums(squares) * (1.0 / features)
    scale = lax.rsqrt(var + NORM_EPS)
    for b in range(count):
        gain = gain_of(b).astype(jnp.float32)
        normed_ref[:, b * breadth : (b + 1) * breadth] = ((block_of(b) - mean) * scale * gain).astype(
            jnp.bfloat16
        )
    projected = jnp.zeros((rows, 3 * HD), jnp.float32)
    for c in range(CHUNKS):
        w_ref = weights_of(c)
        side_by_side = jnp.concatenate([w_ref[j, c * step : (c + 1) * step, :] for j in range(3)], axis=1)
        projected = projected + jnp.dot(
            normed_ref[:, c * step : (c + 1) * step], side_by_side, preferred_element_type=jnp.float32
        )
    projected = projected.astype(jnp.bfloat16)
    queries, keys, values = projected[:, :HD], projected[:, HD : 2 * HD], projected[:, 2 * HD :]
    scores = lax.dot_general(
        queries, keys, (((1,), (1,)), ((), ())), preferred_element_type=jnp.float32
    ) * HD ** (-0.5)
    causal = lax.broadcasted_iota(jnp.int32, scores.shape, 0) >= lax.broadcasted_iota(
        jnp.int32, scores.shape, 1
    )
    scores = jnp.where(causal, scores, -jnp.inf)
    weights = jnp.exp(scores - jnp.max(scores, axis=-1, keepdims=True))
    probs = (weights / jnp.sum(weights, axis=-1, keepdims=True)).astype(jnp.bfloat16)
    return jnp.dot(probs, values, preferred_element_type=jnp.float32).astype(jnp.bfloat16)


def opening_kernel(
    lost_hbm, plan_hbm, x_hbm, gain_hbm, w_hbm, mix_hbm, out_ref, x_sh_ref, facts_ref, x_ref, gain_ref, normed_ref, w_ref, lost_ref, plan_ref, sems, x_sems, w_sems, mix_sems
):
    count = out_ref.shape[0]
    rows, features = x_ref.shape
    breadth = features // count
    step = features // CHUNKS
    x_copies = [
        pltpu.make_async_copy(
            x_hbm.at[:, pl.ds(c * step, step)], x_ref.at[:, pl.ds(c * step, step)], x_sems.at[c]
        )
        for c in range(CHUNKS)
    ]
    gain_copy = pltpu.make_async_copy(gain_hbm, gain_ref, sems.at[0])
    lost_copy = pltpu.make_async_copy(lost_hbm, lost_ref, sems.at[1])
    plan_copy = pltpu.make_async_copy(plan_hbm, plan_ref, sems.at[2])
    w_copies = [
        pltpu.make_async_copy(
            w_hbm.at[:, pl.ds(c * step, step), :], w_ref.at[:, pl.ds(c * step, step), :], w_sems.at[c]
        )
        for c in range(CHUNKS)
    ]
    mix_copies = [
        pltpu.make_async_copy(
            mix_hbm.at[:, pl.ds(b * breadth, breadth)], out_ref.at[b, :, pl.ds(0, breadth)], mix_sems.at[b]
        )
        for b in range(count)
    ]
    for copy in [lost_copy, plan_copy, *x_copies, gain_copy, *w_copies, *mix_copies]:
        copy.start()
    lost_copy.wait()
    plan_copy.wait()
    facts_ref[0] = lost_ref[0]
    for t in range(TICKS):
        facts_ref[t + 1] = plan_ref[t]
    dead = lost_ref[0] == lax.axis_index("section")

    def block_of(b):
        block = x_ref[:, b * breadth : (b + 1) * breadth].astype(jnp.float32)
        return jnp.where(dead, 0.0, block)

    def weights_of(c):
        w_copies[c].wait()
        return w_ref

    def gain_of(b):
        return gain_ref[:, b * breadth : (b + 1) * breadth]

    for copy in [*x_copies, gain_copy]:
        copy.wait()
    context = head_context(block_of, count, breadth, gain_of, weights_of, normed_ref)
    for b in range(count):
        out_ref[b, :, breadth:] = context
    start = pl.multiple_of(lax.axis_index("tp") * breadth, breadth)
    x_sh = x_ref[:, pl.ds(start, breadth)]
    x_sh_ref[...] = jnp.where(dead, jnp.zeros_like(x_sh), x_sh)
    for copy in mix_copies:
        copy.wait()


def phase_kernel(x_ref, pack_ref, w_ref, out_ref, normed_ref):
    count, _, breadth = x_ref.shape

    def gain_of(b):
        return pack_ref[count, b : b + 1, :]

    context = head_context(
        lambda b: x_ref[b].astype(jnp.float32), count, breadth, gain_of, lambda c: w_ref, normed_ref
    )
    for b in range(count):
        out_ref[b] = context


def mix_kernel(x_ref, heads_ref, mixed_ref, out_ref):
    branch = jnp.zeros(x_ref.shape, jnp.float32)
    for h in range(heads_ref.shape[0]):
        branch = branch + jnp.dot(heads_ref[h], mixed_ref[h], preferred_element_type=jnp.float32)
    out_ref[...] = (x_ref[...].astype(jnp.float32) + branch).astype(jnp.bfloat16)


def first_mix_kernel(x_ref, joint_ref, gain_ref, out_ref, pack_ref):
    count, breadth = joint_ref.shape[0], x_ref.shape[1]
    branch = jnp.zeros(x_ref.shape, jnp.float32)
    for h in range(count):
        branch = branch + jnp.dot(
            joint_ref[h, :, breadth:], joint_ref[h, :, :breadth], preferred_element_type=jnp.float32
        )
    out_ref[...] = (x_ref[...].astype(jnp.float32) + branch).astype(jnp.bfloat16)
    for h in range(count):
        pack_ref[h] = joint_ref[h, :, :breadth]
    pack_ref[count] = jnp.zeros(x_ref.shape, jnp.bfloat16)
    for b in range(count):
        pack_ref[count, b : b + 1] = gain_ref[:, b * breadth : (b + 1) * breadth]


def lost_near_end(lost, sections):
    return (lost == sections - 2) | (lost == sections - 3)


def enter_kernel(following, facts_ref, moved_ref, stayed_ref, pool_ref, kept_ref, x_ref, copies_ref, keep_ref):
    sections, mine, lost = lax.axis_size("section"), lax.axis_index("section"), facts_ref[0]
    late = lost_near_end(lost, sections)
    phase = following - 1
    rows = jnp.where(mine % 2 == phase % 2, moved_ref[...], stayed_ref[...])
    if keep_ref is not None:
        before = (mine + sections - 1) % sections
        ahead = before - lost
        if phase == 2:
            here = (before != 0) & (ahead == 1)
        else:
            here = jnp.where(before == 0, ~late, (ahead < 1) | (ahead > 3))
        kept = jnp.zeros_like(rows) if kept_ref is None else kept_ref[...]
        keep_ref[...] = jnp.where(here, rows, kept)
    first = mine == (0 if following % 2 == 1 else 1)
    if following == 4:
        first = first & late
    if following == 5:
        first = first & ~late
    rows = jnp.where(first, pool_ref[facts_ref[min(following - 1, TICKS)]], rows)
    if following == 3:
        rows = jnp.where((mine == lost) & (lost == sections - 1), jnp.zeros_like(rows), rows)
    x_ref[...] = rows
    for b in range(copies_ref.shape[0]):
        copies_ref[b] = rows


def later_kernel(facts_ref, fifth_ref, fourth_ref, out_ref):
    sections, mine, lost = lax.axis_size("section"), lax.axis_index("section"), facts_ref[0]
    count, _, breadth = fifth_ref.shape
    behind = mine - lost
    late = lost_near_end(lost, sections)
    second = ((mine == 0) & ~late) | ((mine != 0) & (behind >= 1) & (behind <= 3))

    def store(block_of):
        for b in range(count):
            out_ref[:, b * breadth : (b + 1) * breadth] = block_of(b)

    @pl.when(mine == lost)
    def _():
        store(lambda b: jnp.zeros(fifth_ref.shape[1:], jnp.bfloat16))

    @pl.when((mine != lost) & second)
    def _():
        store(lambda b: fifth_ref[b])

    @pl.when((mine != lost) & ~second)
    def _():
        store(lambda b: fourth_ref[b])


def standby_kernel(facts_ref, arrived_ref, kept_ref, out_ref):
    sections, mine, lost = lax.axis_size("section"), lax.axis_index("section"), facts_ref[0]
    before = (mine + sections - 1) % sections
    ahead = before - lost
    here = ((before == 0) & lost_near_end(lost, sections)) | ((before != 0) & (ahead >= 2) & (ahead <= 3))
    out_ref[...] = jnp.where(here, arrived_ref[...], kept_ref[...])


VMEM = pl.BlockSpec(memory_space=pltpu.VMEM)
SMEM = pl.BlockSpec(memory_space=pltpu.SMEM)
HBM = pl.BlockSpec(memory_space=pltpu.HBM)
LIMIT = pltpu.CompilerParams(vmem_limit_bytes=16 * 1024 * 1024)
WHOLE = pltpu.CompilerParams(vmem_limit_bytes=57 * 1024 * 1024)


def opening(lost, plan, x_full, gain, w_in, mixing, members):
    rows, features = x_full.shape
    breadth = features // members
    return pl.pallas_call(
        opening_kernel,
        out_shape=[
            pltpu.VMEM((members, rows, breadth + HD), jnp.bfloat16),
            pltpu.VMEM((rows, breadth), jnp.bfloat16),
            pltpu.SMEM((TICKS + 1,), jnp.int32),
        ],
        in_specs=[HBM] * 6,
        out_specs=[VMEM, VMEM, SMEM],
        scratch_shapes=[
            pltpu.VMEM((rows, features), jnp.bfloat16),
            pltpu.VMEM((1, features), jnp.bfloat16),
            pltpu.VMEM((rows, features), jnp.bfloat16),
            pltpu.VMEM((3, features, HD), jnp.bfloat16),
            pltpu.SMEM(lost.shape, jnp.int32),
            pltpu.SMEM(plan.shape, jnp.int32),
            pltpu.SemaphoreType.DMA((3,)),
            pltpu.SemaphoreType.DMA((CHUNKS,)),
            pltpu.SemaphoreType.DMA((CHUNKS,)),
            pltpu.SemaphoreType.DMA((members,)),
        ],
        compiler_params=WHOLE,
        name="opening",
    )(lost, plan, x_full, gain, w_in, mixing)


def contexts(x_blocks, pack, w_in):
    members, rows, breadth = x_blocks.shape
    return pl.pallas_call(
        phase_kernel,
        out_shape=jax.ShapeDtypeStruct((members, rows, HD), jnp.bfloat16),
        in_specs=[VMEM, VMEM, VMEM],
        out_specs=VMEM,
        scratch_shapes=[pltpu.VMEM((rows, members * breadth), jnp.bfloat16)],
        compiler_params=LIMIT,
        name="contexts",
    )(x_blocks, pack, w_in)


def mixed_rows(x_sh, heads, mixed):
    return pl.pallas_call(
        mix_kernel,
        out_shape=jax.ShapeDtypeStruct(x_sh.shape, jnp.bfloat16),
        in_specs=[VMEM, VMEM, VMEM],
        out_specs=VMEM,
        compiler_params=LIMIT,
        name="mixed_rows",
    )(x_sh, heads, mixed)


def first_mixed_rows(x_sh, joint, gain):
    members, rows, _ = joint.shape
    return pl.pallas_call(
        first_mix_kernel,
        out_shape=[
            jax.ShapeDtypeStruct(x_sh.shape, jnp.bfloat16),
            jax.ShapeDtypeStruct((members + 1, rows, x_sh.shape[1]), jnp.bfloat16),
        ],
        in_specs=[VMEM, VMEM, VMEM],
        out_specs=[VMEM, VMEM],
        compiler_params=LIMIT,
        name="first_mixed_rows",
    )(x_sh, joint, gain)


def entering_rows(following, facts, moved_rows, stayed_rows, pool, kept, members):
    keeps = following % 2 == 1
    operands = [facts, moved_rows, stayed_rows, pool]
    if kept is not None:
        operands.append(kept)
    shape = jax.ShapeDtypeStruct(stayed_rows.shape, jnp.bfloat16)
    copies = jax.ShapeDtypeStruct((members, *stayed_rows.shape), jnp.bfloat16)

    def body(*refs):
        inputs, outputs = list(refs[: len(operands)]), list(refs[len(operands) :])
        if kept is None:
            inputs.append(None)
        if not keeps:
            outputs.append(None)
        enter_kernel(following, *inputs, *outputs)

    return pl.pallas_call(
        body,
        out_shape=[shape, copies] + [shape] * keeps,
        in_specs=[SMEM] + [VMEM] * (len(operands) - 1),
        out_specs=[VMEM] * (2 + keeps),
        compiler_params=LIMIT,
        name="entering_rows",
    )(*operands)


def later_rows(facts, fifth, fourth):
    members, rows, breadth = fifth.shape
    return pl.pallas_call(
        later_kernel,
        out_shape=jax.ShapeDtypeStruct((rows, members * breadth), jnp.bfloat16),
        in_specs=[SMEM, VMEM, VMEM],
        out_specs=VMEM,
        compiler_params=LIMIT,
        name="later_rows",
    )(facts, fifth, fourth)


def standby_rows(facts, arrived, kept):
    return pl.pallas_call(
        standby_kernel,
        out_shape=jax.ShapeDtypeStruct(kept.shape, jnp.bfloat16),
        in_specs=[SMEM, VMEM, VMEM],
        out_specs=VMEM,
        compiler_params=LIMIT,
        name="standby_rows",
    )(facts, arrived, kept)


def per_device(
    pending_activation,
    admissible_microbatches,
    arrival_plan,
    vanished_hop,
    query_key_value_matrices,
    mixing_projection_matrices,
    normalizer_factors,
):
    members = lax.axis_size("tp")
    w_in = jnp.moveaxis(query_key_value_matrices[0], 1, 0)
    other_w = swapped(w_in, "section")
    sent, x_sh, facts = opening(
        vanished_hop,
        arrival_plan,
        pending_activation[0],
        normalizer_factors,
        w_in,
        mixing_projection_matrices[0],
        members,
    )
    y_sh, pack = first_mixed_rows(x_sh, exchange(sent, "tp"), normalizer_factors)
    other_pack = swapped(pack, "section")

    kept = None
    for following in range(2, PHASES + 1):
        moved_rows = moved(y_sh, "section", (following - 1) % 2, following == 2)
        x_sh, copies, *keep = entering_rows(
            following, facts, moved_rows, y_sh, admissible_microbatches, kept, members
        )
        if keep:
            kept = keep[0]
        if following == PHASES:
            copies, fourth = lax.optimization_barrier((copies, fourth))
        x_blocks = exchange(copies, "tp")
        if following == PHASES - 1:
            fourth = swapped(x_blocks, "section")
        layer_w, layer_pack = (w_in, pack) if following % 2 == 1 else (other_w, other_pack)
        heads = exchange(contexts(x_blocks, layer_pack, layer_w), "tp")
        y_sh = mixed_rows(x_sh, heads, layer_pack)
    y_sh, x_blocks, fourth = lax.optimization_barrier((y_sh, x_blocks, fourth))
    arrived = shifted(y_sh, "section", 1)
    later = later_rows(facts, x_blocks, fourth)
    return (later[None], standby_rows(facts, arrived, kept)[None])


def solution(mesh):
    placed = (
        P("section", None, None),
        P(None, None, "tp"),
        P(),
        P(),
        P("section", None, None, "tp"),
        P("section", "tp", None),
        P("section", None),
    )
    return jax.shard_map(
        per_device,
        mesh=mesh,
        in_specs=placed,
        out_specs=(P("section", None, None), P("section", None, "tp")),
        check_vma=False,
    )
```

```python
import jax
import jax.numpy as jnp
from jax import lax
from jax.experimental import pallas as pl
from jax.experimental.pallas import tpu as pltpu
from jax.sharding import PartitionSpec as P

HD = 128
TICKS = 3
PHASES = TICKS + 2

NORM_EPS = 1e-05
CHUNKS = 1


def shifted(value, axis, steps):
    count = lax.axis_size(axis)
    pairs = [(source, (source + steps) % count) for source in range(count)]
    return lax.ppermute(value, axis, pairs)


def moved(value, axis, parity, drop=False):
    count = lax.axis_size(axis)
    pairs = [((target - 2) % count, target) for target in range(count) if target % 2 == parity]
    if drop:
        pairs = [pair for pair in pairs if pair[1] != 1]
    return lax.ppermute(value, axis, pairs)


def swapped(value, axis):
    return lax.ppermute(value, axis, [(s, s + 1 - 2 * (s % 2)) for s in range(lax.axis_size(axis))])


def exchange(blocks, axis):
    return lax.all_to_all(blocks, axis, split_axis=0, concat_axis=0, tiled=True)


def head_context(block_of, count, breadth, gain_of, weights_of, normed_ref):
    features = count * breadth
    step = features // CHUNKS
    rows = normed_ref.shape[0]

    def row_sums(values_of):
        total = jnp.zeros((rows, HD), jnp.float32)
        for b in range(count):
            value = values_of(b)
            for c in range(breadth // HD):
                total = total + value[:, c * HD : (c + 1) * HD]
        return jnp.sum(total, axis=-1, keepdims=True)

    mean = row_sums(block_of) * (1.0 / features)

    def squares(b):
        centered = block_of(b) - mean
        return centered * centered

    var = row_sums(squares) * (1.0 / features)
    scale = lax.rsqrt(var + NORM_EPS)
    for b in range(count):
        gain = gain_of(b).astype(jnp.float32)
        normed_ref[:, b * breadth : (b + 1) * breadth] = ((block_of(b) - mean) * scale * gain).astype(
            jnp.bfloat16
        )
    projected = jnp.zeros((rows, 3 * HD), jnp.float32)
    for c in range(CHUNKS):
        w_ref = weights_of(c)
        side_by_side = jnp.concatenate([w_ref[j, c * step : (c + 1) * step, :] for j in range(3)], axis=1)
        projected = projected + jnp.dot(
            normed_ref[:, c * step : (c + 1) * step], side_by_side, preferred_element_type=jnp.float32
        )
    projected = projected.astype(jnp.bfloat16)
    queries, keys, values = projected[:, :HD], projected[:, HD : 2 * HD], projected[:, 2 * HD :]
    scores = lax.dot_general(
        queries, keys, (((1,), (1,)), ((), ())), preferred_element_type=jnp.float32
    ) * HD ** (-0.5)
    causal = lax.broadcasted_iota(jnp.int32, scores.shape, 0) >= lax.broadcasted_iota(
        jnp.int32, scores.shape, 1
    )
    scores = jnp.where(causal, scores, -jnp.inf)
    weights = jnp.exp(scores - jnp.max(scores, axis=-1, keepdims=True))
    probs = (weights / jnp.sum(weights, axis=-1, keepdims=True)).astype(jnp.bfloat16)
    return jnp.dot(probs, values, preferred_element_type=jnp.float32).astype(jnp.bfloat16)


def opening_kernel(
    lost_hbm, plan_hbm, x_hbm, gain_hbm, w_hbm, mix_hbm, out_ref, x_sh_ref, facts_ref, x_ref, gain_ref, normed_ref, w_ref, lost_ref, plan_ref, sems, x_sems, w_sems, mix_sems
):
    count = out_ref.shape[0]
    rows, features = x_ref.shape
    breadth = features // count
    step = features // CHUNKS
    x_copies = [
        pltpu.make_async_copy(
            x_hbm.at[:, pl.ds(c * step, step)], x_ref.at[:, pl.ds(c * step, step)], x_sems.at[c]
        )
        for c in range(CHUNKS)
    ]
    gain_copy = pltpu.make_async_copy(gain_hbm, gain_ref, sems.at[0])
    lost_copy = pltpu.make_async_copy(lost_hbm, lost_ref, sems.at[1])
    plan_copy = pltpu.make_async_copy(plan_hbm, plan_ref, sems.at[2])
    w_copies = [
        pltpu.make_async_copy(
            w_hbm.at[:, pl.ds(c * step, step), :], w_ref.at[:, pl.ds(c * step, step), :], w_sems.at[c]
        )
        for c in range(CHUNKS)
    ]
    mix_copies = [
        pltpu.make_async_copy(
            mix_hbm.at[:, pl.ds(b * breadth, breadth)], out_ref.at[b, :, pl.ds(0, breadth)], mix_sems.at[b]
        )
        for b in range(count)
    ]
    for copy in [lost_copy, plan_copy, *x_copies, gain_copy, *w_copies, *mix_copies]:
        copy.start()
    lost_copy.wait()
    plan_copy.wait()
    facts_ref[0] = lost_ref[0]
    for t in range(TICKS):
        facts_ref[t + 1] = plan_ref[t]
    dead = lost_ref[0] == lax.axis_index("section")

    def block_of(b):
        block = x_ref[:, b * breadth : (b + 1) * breadth].astype(jnp.float32)
        return jnp.where(dead, 0.0, block)

    def weights_of(c):
        w_copies[c].wait()
        return w_ref

    def gain_of(b):
        return gain_ref[:, b * breadth : (b + 1) * breadth]

    for copy in [*x_copies, gain_copy]:
        copy.wait()
    context = head_context(block_of, count, breadth, gain_of, weights_of, normed_ref)
    for b in range(count):
        out_ref[b, :, breadth:] = context
    start = pl.multiple_of(lax.axis_index("tp") * breadth, breadth)
    x_sh = x_ref[:, pl.ds(start, breadth)]
    x_sh_ref[...] = jnp.where(dead, jnp.zeros_like(x_sh), x_sh)
    for copy in mix_copies:
        copy.wait()


def phase_kernel(x_ref, pack_ref, w_ref, out_ref, normed_ref):
    count, _, breadth = x_ref.shape

    def gain_of(b):
        return pack_ref[count, b : b + 1, :]

    context = head_context(
        lambda b: x_ref[b].astype(jnp.float32), count, breadth, gain_of, lambda c: w_ref, normed_ref
    )
    for b in range(count):
        out_ref[b] = context


def mix_kernel(x_ref, heads_ref, mixed_ref, out_ref):
    branch = jnp.zeros(x_ref.shape, jnp.float32)
    for h in range(heads_ref.shape[0]):
        branch = branch + jnp.dot(heads_ref[h], mixed_ref[h], preferred_element_type=jnp.float32)
    out_ref[...] = (x_ref[...].astype(jnp.float32) + branch).astype(jnp.bfloat16)


def first_mix_kernel(x_ref, joint_ref, gain_ref, out_ref, pack_ref):
    count, breadth = joint_ref.shape[0], x_ref.shape[1]
    branch = jnp.zeros(x_ref.shape, jnp.float32)
    for h in range(count):
        branch = branch + jnp.dot(
            joint_ref[h, :, breadth:], joint_ref[h, :, :breadth], preferred_element_type=jnp.float32
        )
    out_ref[...] = (x_ref[...].astype(jnp.float32) + branch).astype(jnp.bfloat16)
    for h in range(count):
        pack_ref[h] = joint_ref[h, :, :breadth]
    pack_ref[count] = jnp.zeros(x_ref.shape, jnp.bfloat16)
    for b in range(count):
        pack_ref[count, b : b + 1] = gain_ref[:, b * breadth : (b + 1) * breadth]


def lost_near_end(lost, sections):
    return (lost == sections - 2) | (lost == sections - 3)


def enter_kernel(following, facts_ref, moved_ref, stayed_ref, pool_ref, kept_ref, x_ref, copies_ref, keep_ref):
    sections, mine, lost = lax.axis_size("section"), lax.axis_index("section"), facts_ref[0]
    late = lost_near_end(lost, sections)
    phase = following - 1
    rows = jnp.where(mine % 2 == phase % 2, moved_ref[...], stayed_ref[...])
    if keep_ref is not None:
        before = (mine + sections - 1) % sections
        ahead = before - lost
        if phase == 2:
            here = (before != 0) & (ahead == 1)
        else:
            here = jnp.where(before == 0, ~late, (ahead < 1) | (ahead > 3))
        kept = jnp.zeros_like(rows) if kept_ref is None else kept_ref[...]
        keep_ref[...] = jnp.where(here, rows, kept)
    first = mine == (0 if following % 2 == 1 else 1)
    if following == 4:
        first = first & late
    if following == 5:
        first = first & ~late
    rows = jnp.where(first, pool_ref[facts_ref[min(following - 1, TICKS)]], rows)
    if following == 3:
        rows = jnp.where((mine == lost) & (lost == sections - 1), jnp.zeros_like(rows), rows)
    x_ref[...] = rows
    for b in range(copies_ref.shape[0]):
        copies_ref[b] = rows


def later_kernel(facts_ref, fifth_ref, fourth_ref, out_ref):
    sections, mine, lost = lax.axis_size("section"), lax.axis_index("section"), facts_ref[0]
    count, _, breadth = fifth_ref.shape
    behind = mine - lost
    late = lost_near_end(lost, sections)
    second = ((mine == 0) & ~late) | ((mine != 0) & (behind >= 1) & (behind <= 3))

    def store(block_of):
        for b in range(count):
            out_ref[:, b * breadth : (b + 1) * breadth] = block_of(b)

    @pl.when(mine == lost)
    def _():
        store(lambda b: jnp.zeros(fifth_ref.shape[1:], jnp.bfloat16))

    @pl.when((mine != lost) & second)
    def _():
        store(lambda b: fifth_ref[b])

    @pl.when((mine != lost) & ~second)
    def _():
        store(lambda b: fourth_ref[b])


def standby_kernel(facts_ref, arrived_ref, kept_ref, out_ref):
    sections, mine, lost = lax.axis_size("section"), lax.axis_index("section"), facts_ref[0]
    before = (mine + sections - 1) % sections
    ahead = before - lost
    here = ((before == 0) & lost_near_end(lost, sections)) | ((before != 0) & (ahead >= 2) & (ahead <= 3))
    out_ref[...] = jnp.where(here, arrived_ref[...], kept_ref[...])


VMEM = pl.BlockSpec(memory_space=pltpu.VMEM)
SMEM = pl.BlockSpec(memory_space=pltpu.SMEM)
HBM = pl.BlockSpec(memory_space=pltpu.HBM)
LIMIT = pltpu.CompilerParams(vmem_limit_bytes=16 * 1024 * 1024)
WHOLE = pltpu.CompilerParams(vmem_limit_bytes=57 * 1024 * 1024)


def opening(lost, plan, x_full, gain, w_in, mixing, members):
    rows, features = x_full.shape
    breadth = features // members
    return pl.pallas_call(
        opening_kernel,
        out_shape=[
            pltpu.VMEM((members, rows, breadth + HD), jnp.bfloat16),
            pltpu.VMEM((rows, breadth), jnp.bfloat16),
            pltpu.SMEM((TICKS + 1,), jnp.int32),
        ],
        in_specs=[HBM] * 6,
        out_specs=[VMEM, VMEM, SMEM],
        scratch_shapes=[
            pltpu.VMEM((rows, features), jnp.bfloat16),
            pltpu.VMEM((1, features), jnp.bfloat16),
            pltpu.VMEM((rows, features), jnp.bfloat16),
            pltpu.VMEM((3, features, HD), jnp.bfloat16),
            pltpu.SMEM(lost.shape, jnp.int32),
            pltpu.SMEM(plan.shape, jnp.int32),
            pltpu.SemaphoreType.DMA((3,)),
            pltpu.SemaphoreType.DMA((CHUNKS,)),
            pltpu.SemaphoreType.DMA((CHUNKS,)),
            pltpu.SemaphoreType.DMA((members,)),
        ],
        compiler_params=WHOLE,
        name="opening",
    )(lost, plan, x_full, gain, w_in, mixing)


def contexts(x_blocks, pack, w_in):
    members, rows, breadth = x_blocks.shape
    return pl.pallas_call(
        phase_kernel,
        out_shape=jax.ShapeDtypeStruct((members, rows, HD), jnp.bfloat16),
        in_specs=[VMEM, VMEM, VMEM],
        out_specs=VMEM,
        scratch_shapes=[pltpu.VMEM((rows, members * breadth), jnp.bfloat16)],
        compiler_params=LIMIT,
        name="contexts",
    )(x_blocks, pack, w_in)


def mixed_rows(x_sh, heads, mixed):
    return pl.pallas_call(
        mix_kernel,
        out_shape=jax.ShapeDtypeStruct(x_sh.shape, jnp.bfloat16),
        in_specs=[VMEM, VMEM, VMEM],
        out_specs=VMEM,
        compiler_params=LIMIT,
        name="mixed_rows",
    )(x_sh, heads, mixed)


def first_mixed_rows(x_sh, joint, gain):
    members, rows, _ = joint.shape
    return pl.pallas_call(
        first_mix_kernel,
        out_shape=[
            jax.ShapeDtypeStruct(x_sh.shape, jnp.bfloat16),
            jax.ShapeDtypeStruct((members + 1, rows, x_sh.shape[1]), jnp.bfloat16),
        ],
        in_specs=[VMEM, VMEM, VMEM],
        out_specs=[VMEM, VMEM],
        compiler_params=LIMIT,
        name="first_mixed_rows",
    )(x_sh, joint, gain)


def entering_rows(following, facts, moved_rows, stayed_rows, pool, kept, members):
    keeps = following % 2 == 1
    operands = [facts, moved_rows, stayed_rows, pool]
    if kept is not None:
        operands.append(kept)
    shape = jax.ShapeDtypeStruct(stayed_rows.shape, jnp.bfloat16)
    copies = jax.ShapeDtypeStruct((members, *stayed_rows.shape), jnp.bfloat16)

    def body(*refs):
        inputs, outputs = list(refs[: len(operands)]), list(refs[len(operands) :])
        if kept is None:
            inputs.append(None)
        if not keeps:
            outputs.append(None)
        enter_kernel(following, *inputs, *outputs)

    return pl.pallas_call(
        body,
        out_shape=[shape, copies] + [shape] * keeps,
        in_specs=[SMEM] + [VMEM] * (len(operands) - 1),
        out_specs=[VMEM] * (2 + keeps),
        compiler_params=LIMIT,
        name="entering_rows",
    )(*operands)


def later_rows(facts, fifth, fourth):
    members, rows, breadth = fifth.shape
    return pl.pallas_call(
        later_kernel,
        out_shape=jax.ShapeDtypeStruct((rows, members * breadth), jnp.bfloat16),
        in_specs=[SMEM, VMEM, VMEM],
        out_specs=VMEM,
        compiler_params=LIMIT,
        name="later_rows",
    )(facts, fifth, fourth)


def standby_rows(facts, arrived, kept):
    return pl.pallas_call(
        standby_kernel,
        out_shape=jax.ShapeDtypeStruct(kept.shape, jnp.bfloat16),
        in_specs=[SMEM, VMEM, VMEM],
        out_specs=VMEM,
        compiler_params=LIMIT,
        name="standby_rows",
    )(facts, arrived, kept)


def per_device(
    pending_activation,
    admissible_microbatches,
    arrival_plan,
    vanished_hop,
    query_key_value_matrices,
    mixing_projection_matrices,
    normalizer_factors,
):
    members = lax.axis_size("tp")
    w_in = jnp.moveaxis(query_key_value_matrices[0], 1, 0)
    other_w = swapped(w_in, "section")
    sent, x_sh, facts = opening(
        vanished_hop,
        arrival_plan,
        pending_activation[0],
        normalizer_factors,
        w_in,
        mixing_projection_matrices[0],
        members,
    )
    y_sh, pack = first_mixed_rows(x_sh, exchange(sent, "tp"), normalizer_factors)
    other_pack = swapped(pack, "section")

    kept = None
    for following in range(2, PHASES + 1):
        moved_rows = moved(y_sh, "section", (following - 1) % 2, following == 2)
        x_sh, copies, *keep = entering_rows(
            following, facts, moved_rows, y_sh, admissible_microbatches, kept, members
        )
        if keep:
            kept = keep[0]
        if following == PHASES:
            copies, fourth = lax.optimization_barrier((copies, fourth))
        x_blocks = exchange(copies, "tp")
        if following == PHASES - 1:
            fourth = swapped(x_blocks, "section")
        layer_w, layer_pack = (w_in, pack) if following % 2 == 1 else (other_w, other_pack)
        heads = exchange(contexts(x_blocks, layer_pack, layer_w), "tp")
        y_sh = mixed_rows(x_sh, heads, layer_pack)
    y_sh, x_blocks, fourth = lax.optimization_barrier((y_sh, x_blocks, fourth))
    arrived = shifted(y_sh, "section", 1)
    later = later_rows(facts, x_blocks, fourth)
    return (later[None], standby_rows(facts, arrived, kept)[None])


def solution(mesh):
    placed = (
        P("section", None, None),
        P(None, None, "tp"),
        P(),
        P(),
        P("section", None, None, "tp"),
        P("section", "tp", None),
        P("section", None),
    )
    return jax.shard_map(
        per_device,
        mesh=mesh,
        in_specs=placed,
        out_specs=(P("section", None, None), P("section", None, "tp")),
        check_vma=False,
    )
```

```python
import jax
import jax.numpy as jnp
from jax import lax
from jax.experimental import pallas as pl
from jax.experimental.pallas import tpu as pltpu
from jax.sharding import PartitionSpec as P

HD = 128
TICKS = 3
PHASES = TICKS + 2

NORM_EPS = 1e-05
CHUNKS = 1


def shifted(value, axis, steps):
    count = lax.axis_size(axis)
    pairs = [(source, (source + steps) % count) for source in range(count)]
    return lax.ppermute(value, axis, pairs)


def moved(value, axis, parity, drop=False):
    count = lax.axis_size(axis)
    pairs = [((target - 2) % count, target) for target in range(count) if target % 2 == parity]
    if drop:
        pairs = [pair for pair in pairs if pair[1] != 1]
    return lax.ppermute(value, axis, pairs)


def swapped(value, axis):
    return lax.ppermute(value, axis, [(s, s + 1 - 2 * (s % 2)) for s in range(lax.axis_size(axis))])


def exchange(blocks, axis):
    return lax.all_to_all(blocks, axis, split_axis=0, concat_axis=0, tiled=True)


def head_context(block_of, count, breadth, gain_of, weights_of, normed_ref):
    features = count * breadth
    step = features // CHUNKS
    rows = normed_ref.shape[0]

    def row_sums(values_of):
        total = jnp.zeros((rows, HD), jnp.float32)
        for b in range(count):
            value = values_of(b)
            total = total + sum(value[:, c * HD : (c + 1) * HD] for c in range(breadth // HD))
        return jnp.sum(total, axis=-1, keepdims=True)

    mean = row_sums(block_of) * (1.0 / features)

    def squares(b):
        centered = block_of(b) - mean
        return centered * centered

    var = row_sums(squares) * (1.0 / features)
    scale = lax.rsqrt(var + NORM_EPS)
    for b in range(count):
        gain = gain_of(b).astype(jnp.float32)
        normed_ref[:, b * breadth : (b + 1) * breadth] = ((block_of(b) - mean) * scale * gain).astype(
            jnp.bfloat16
        )
    projected = jnp.zeros((rows, 3 * HD), jnp.float32)
    for c in range(CHUNKS):
        w_ref = weights_of(c)
        side_by_side = jnp.concatenate([w_ref[j, c * step : (c + 1) * step, :] for j in range(3)], axis=1)
        projected = projected + jnp.dot(
            normed_ref[:, c * step : (c + 1) * step], side_by_side, preferred_element_type=jnp.float32
        )
    projected = projected.astype(jnp.bfloat16)
    queries, keys, values = projected[:, :HD], projected[:, HD : 2 * HD], projected[:, 2 * HD :]
    scores = lax.dot_general(
        queries, keys, (((1,), (1,)), ((), ())), preferred_element_type=jnp.float32
    ) * HD ** (-0.5)
    causal = lax.broadcasted_iota(jnp.int32, scores.shape, 0) >= lax.broadcasted_iota(
        jnp.int32, scores.shape, 1
    )
    scores = jnp.where(causal, scores, -jnp.inf)
    weights = jnp.exp(scores - jnp.max(scores, axis=-1, keepdims=True))
    probs = (weights / jnp.sum(weights, axis=-1, keepdims=True)).astype(jnp.bfloat16)
    return jnp.dot(probs, values, preferred_element_type=jnp.float32).astype(jnp.bfloat16)


def opening_kernel(
    lost_hbm, plan_hbm, x_hbm, gain_hbm, w_hbm, mix_hbm, out_ref, x_sh_ref, facts_ref, x_ref, gain_ref, normed_ref, w_ref, lost_ref, plan_ref, sems, x_sems, w_sems, mix_sems
):
    count = out_ref.shape[0]
    rows, features = x_ref.shape
    breadth = features // count
    step = features // CHUNKS
    x_copies = [
        pltpu.make_async_copy(
            x_hbm.at[:, pl.ds(c * step, step)], x_ref.at[:, pl.ds(c * step, step)], x_sems.at[c]
        )
        for c in range(CHUNKS)
    ]
    gain_copy = pltpu.make_async_copy(gain_hbm, gain_ref, sems.at[0])
    lost_copy = pltpu.make_async_copy(lost_hbm, lost_ref, sems.at[1])
    plan_copy = pltpu.make_async_copy(plan_hbm, plan_ref, sems.at[2])
    w_copies = [
        pltpu.make_async_copy(
            w_hbm.at[:, pl.ds(c * step, step), :], w_ref.at[:, pl.ds(c * step, step), :], w_sems.at[c]
        )
        for c in range(CHUNKS)
    ]
    mix_copies = [
        pltpu.make_async_copy(
            mix_hbm.at[:, pl.ds(b * breadth, breadth)], out_ref.at[b, :, pl.ds(0, breadth)], mix_sems.at[b]
        )
        for b in range(count)
    ]
    for copy in [lost_copy, plan_copy, *x_copies, gain_copy, *w_copies, *mix_copies]:
        copy.start()
    lost_copy.wait()
    plan_copy.wait()
    facts_ref[0] = lost_ref[0]
    for t in range(TICKS):
        facts_ref[t + 1] = plan_ref[t]
    dead = lost_ref[0] == lax.axis_index("section")

    def block_of(b):
        block = x_ref[:, b * breadth : (b + 1) * breadth].astype(jnp.float32)
        return jnp.where(dead, 0.0, block)

    def weights_of(c):
        w_copies[c].wait()
        return w_ref

    def gain_of(b):
        return gain_ref[:, b * breadth : (b + 1) * breadth]

    for copy in [*x_copies, gain_copy]:
        copy.wait()
    context = head_context(block_of, count, breadth, gain_of, weights_of, normed_ref)
    for b in range(count):
        out_ref[b, :, breadth:] = context
    start = pl.multiple_of(lax.axis_index("tp") * breadth, breadth)
    x_sh = x_ref[:, pl.ds(start, breadth)]
    x_sh_ref[...] = jnp.where(dead, jnp.zeros_like(x_sh), x_sh)
    for copy in mix_copies:
        copy.wait()


def phase_kernel(x_ref, pack_ref, w_ref, out_ref, normed_ref):
    count, _, breadth = x_ref.shape

    def gain_of(b):
        return pack_ref[count, b : b + 1, :]

    context = head_context(
        lambda b: x_ref[b].astype(jnp.float32), count, breadth, gain_of, lambda c: w_ref, normed_ref
    )
    for b in range(count):
        out_ref[b] = context


def mix_kernel(x_ref, heads_ref, mixed_ref, out_ref):
    branch = jnp.zeros(x_ref.shape, jnp.float32)
    for h in range(heads_ref.shape[0]):
        branch = branch + jnp.dot(heads_ref[h], mixed_ref[h], preferred_element_type=jnp.float32)
    out_ref[...] = (x_ref[...].astype(jnp.float32) + branch).astype(jnp.bfloat16)


def first_mix_kernel(x_ref, joint_ref, gain_ref, out_ref, pack_ref):
    count, breadth = joint_ref.shape[0], x_ref.shape[1]
    branch = jnp.zeros(x_ref.shape, jnp.float32)
    for h in range(count):
        branch = branch + jnp.dot(
            joint_ref[h, :, breadth:], joint_ref[h, :, :breadth], preferred_element_type=jnp.float32
        )
    out_ref[...] = (x_ref[...].astype(jnp.float32) + branch).astype(jnp.bfloat16)
    for h in range(count):
        pack_ref[h] = joint_ref[h, :, :breadth]
    pack_ref[count] = jnp.zeros(x_ref.shape, jnp.bfloat16)
    for b in range(count):
        pack_ref[count, b : b + 1] = gain_ref[:, b * breadth : (b + 1) * breadth]


def lost_near_end(lost, sections):
    return (lost == sections - 2) | (lost == sections - 3)


def enter_kernel(following, facts_ref, moved_ref, stayed_ref, pool_ref, kept_ref, x_ref, copies_ref, keep_ref):
    sections, mine, lost = lax.axis_size("section"), lax.axis_index("section"), facts_ref[0]
    late = lost_near_end(lost, sections)
    phase = following - 1
    rows = jnp.where(mine % 2 == phase % 2, moved_ref[...], stayed_ref[...])
    if keep_ref is not None:
        before = (mine + sections - 1) % sections
        ahead = before - lost
        if phase == 2:
            here = (before != 0) & (ahead == 1)
        else:
            here = jnp.where(before == 0, ~late, (ahead < 1) | (ahead > 3))
        kept = jnp.zeros_like(rows) if kept_ref is None else kept_ref[...]
        keep_ref[...] = jnp.where(here, rows, kept)
    first = mine == (0 if following % 2 == 1 else 1)
    if following == 4:
        first = first & late
    if following == 5:
        first = first & ~late
    rows = jnp.where(first, pool_ref[facts_ref[min(following - 1, TICKS)]], rows)
    if following == 3:
        rows = jnp.where((mine == lost) & (lost == sections - 1), jnp.zeros_like(rows), rows)
    x_ref[...] = rows
    for b in range(copies_ref.shape[0]):
        copies_ref[b] = rows


def later_kernel(facts_ref, fifth_ref, fourth_ref, out_ref):
    sections, mine, lost = lax.axis_size("section"), lax.axis_index("section"), facts_ref[0]
    count, _, breadth = fifth_ref.shape
    behind = mine - lost
    late = lost_near_end(lost, sections)
    second = ((mine == 0) & ~late) | ((mine != 0) & (behind >= 1) & (behind <= 3))

    def store(block_of):
        for b in range(count):
            out_ref[:, b * breadth : (b + 1) * breadth] = block_of(b)

    @pl.when(mine == lost)
    def _():
        store(lambda b: jnp.zeros(fifth_ref.shape[1:], jnp.bfloat16))

    @pl.when((mine != lost) & second)
    def _():
        store(lambda b: fifth_ref[b])

    @pl.when((mine != lost) & ~second)
    def _():
        store(lambda b: fourth_ref[b])


def standby_kernel(facts_ref, arrived_ref, kept_ref, out_ref):
    sections, mine, lost = lax.axis_size("section"), lax.axis_index("section"), facts_ref[0]
    before = (mine + sections - 1) % sections
    ahead = before - lost
    here = ((before == 0) & lost_near_end(lost, sections)) | ((before != 0) & (ahead >= 2) & (ahead <= 3))
    out_ref[...] = jnp.where(here, arrived_ref[...], kept_ref[...])


VMEM = pl.BlockSpec(memory_space=pltpu.VMEM)
SMEM = pl.BlockSpec(memory_space=pltpu.SMEM)
HBM = pl.BlockSpec(memory_space=pltpu.HBM)
LIMIT = pltpu.CompilerParams(vmem_limit_bytes=16 * 1024 * 1024)
WHOLE = pltpu.CompilerParams(vmem_limit_bytes=57 * 1024 * 1024)


def opening(lost, plan, x_full, gain, w_in, mixing, members):
    rows, features = x_full.shape
    breadth = features // members
    return pl.pallas_call(
        opening_kernel,
        out_shape=[
            pltpu.VMEM((members, rows, breadth + HD), jnp.bfloat16),
            pltpu.VMEM((rows, breadth), jnp.bfloat16),
            pltpu.SMEM((TICKS + 1,), jnp.int32),
        ],
        in_specs=[HBM] * 6,
        out_specs=[VMEM, VMEM, SMEM],
        scratch_shapes=[
            pltpu.VMEM((rows, features), jnp.bfloat16),
            pltpu.VMEM((1, features), jnp.bfloat16),
            pltpu.VMEM((rows, features), jnp.bfloat16),
            pltpu.VMEM((3, features, HD), jnp.bfloat16),
            pltpu.SMEM(lost.shape, jnp.int32),
            pltpu.SMEM(plan.shape, jnp.int32),
            pltpu.SemaphoreType.DMA((3,)),
            pltpu.SemaphoreType.DMA((CHUNKS,)),
            pltpu.SemaphoreType.DMA((CHUNKS,)),
            pltpu.SemaphoreType.DMA((members,)),
        ],
        compiler_params=WHOLE,
        name="opening",
    )(lost, plan, x_full, gain, w_in, mixing)


def contexts(x_blocks, pack, w_in):
    members, rows, breadth = x_blocks.shape
    return pl.pallas_call(
        phase_kernel,
        out_shape=jax.ShapeDtypeStruct((members, rows, HD), jnp.bfloat16),
        in_specs=[VMEM, VMEM, VMEM],
        out_specs=VMEM,
        scratch_shapes=[pltpu.VMEM((rows, members * breadth), jnp.bfloat16)],
        compiler_params=LIMIT,
        name="contexts",
    )(x_blocks, pack, w_in)


def mixed_rows(x_sh, heads, mixed):
    return pl.pallas_call(
        mix_kernel,
        out_shape=jax.ShapeDtypeStruct(x_sh.shape, jnp.bfloat16),
        in_specs=[VMEM, VMEM, VMEM],
        out_specs=VMEM,
        compiler_params=LIMIT,
        name="mixed_rows",
    )(x_sh, heads, mixed)


def first_mixed_rows(x_sh, joint, gain):
    members, rows, _ = joint.shape
    return pl.pallas_call(
        first_mix_kernel,
        out_shape=[
            jax.ShapeDtypeStruct(x_sh.shape, jnp.bfloat16),
            jax.ShapeDtypeStruct((members + 1, rows, x_sh.shape[1]), jnp.bfloat16),
        ],
        in_specs=[VMEM, VMEM, VMEM],
        out_specs=[VMEM, VMEM],
        compiler_params=LIMIT,
        name="first_mixed_rows",
    )(x_sh, joint, gain)


def entering_rows(following, facts, moved_rows, stayed_rows, pool, kept, members):
    keeps = following % 2 == 1
    operands = [facts, moved_rows, stayed_rows, pool]
    if kept is not None:
        operands.append(kept)
    shape = jax.ShapeDtypeStruct(stayed_rows.shape, jnp.bfloat16)
    copies = jax.ShapeDtypeStruct((members, *stayed_rows.shape), jnp.bfloat16)

    def body(*refs):
        inputs, outputs = list(refs[: len(operands)]), list(refs[len(operands) :])
        if kept is None:
            inputs.append(None)
        if not keeps:
            outputs.append(None)
        enter_kernel(following, *inputs, *outputs)

    return pl.pallas_call(
        body,
        out_shape=[shape, copies] + [shape] * keeps,
        in_specs=[SMEM] + [VMEM] * (len(operands) - 1),
        out_specs=[VMEM] * (2 + keeps),
        compiler_params=LIMIT,
        name="entering_rows",
    )(*operands)


def later_rows(facts, fifth, fourth):
    members, rows, breadth = fifth.shape
    return pl.pallas_call(
        later_kernel,
        out_shape=jax.ShapeDtypeStruct((rows, members * breadth), jnp.bfloat16),
        in_specs=[SMEM, VMEM, VMEM],
        out_specs=VMEM,
        compiler_params=LIMIT,
        name="later_rows",
    )(facts, fifth, fourth)


def standby_rows(facts, arrived, kept):
    return pl.pallas_call(
        standby_kernel,
        out_shape=jax.ShapeDtypeStruct(kept.shape, jnp.bfloat16),
        in_specs=[SMEM, VMEM, VMEM],
        out_specs=VMEM,
        compiler_params=LIMIT,
        name="standby_rows",
    )(facts, arrived, kept)


def per_device(
    pending_activation,
    admissible_microbatches,
    arrival_plan,
    vanished_hop,
    query_key_value_matrices,
    mixing_projection_matrices,
    normalizer_factors,
):
    members = lax.axis_size("tp")
    w_in = jnp.moveaxis(query_key_value_matrices[0], 1, 0)
    other_w = swapped(w_in, "section")
    sent, x_sh, facts = opening(
        vanished_hop,
        arrival_plan,
        pending_activation[0],
        normalizer_factors,
        w_in,
        mixing_projection_matrices[0],
        members,
    )
    y_sh, pack = first_mixed_rows(x_sh, exchange(sent, "tp"), normalizer_factors)
    other_pack = swapped(pack, "section")

    kept = None
    for following in range(2, PHASES + 1):
        moved_rows = moved(y_sh, "section", (following - 1) % 2, following == 2)
        x_sh, copies, *keep = entering_rows(
            following, facts, moved_rows, y_sh, admissible_microbatches, kept, members
        )
        if keep:
            kept = keep[0]
        if following == PHASES:
            copies, fourth = lax.optimization_barrier((copies, fourth))
        x_blocks = exchange(copies, "tp")
        if following == PHASES - 1:
            fourth = swapped(x_blocks, "section")
        layer_w, layer_pack = (w_in, pack) if following % 2 == 1 else (other_w, other_pack)
        heads = exchange(contexts(x_blocks, layer_pack, layer_w), "tp")
        y_sh = mixed_rows(x_sh, heads, layer_pack)
    y_sh, x_blocks, fourth = lax.optimization_barrier((y_sh, x_blocks, fourth))
    arrived = shifted(y_sh, "section", 1)
    later = later_rows(facts, x_blocks, fourth)
    return (later[None], standby_rows(facts, arrived, kept)[None])


def solution(mesh):
    placed = (
        P("section", None, None),
        P(None, None, "tp"),
        P(),
        P(),
        P("section", None, None, "tp"),
        P("section", "tp", None),
        P("section", None),
    )
    return jax.shard_map(
        per_device,
        mesh=mesh,
        in_specs=placed,
        out_specs=(P("section", None, None), P("section", None, "tp")),
        check_vma=False,
    )
```

```python
import jax
import jax.numpy as jnp
from jax import lax
from jax.experimental import pallas as pl
from jax.experimental.pallas import tpu as pltpu
from jax.sharding import PartitionSpec as P

HD = 128
TICKS = 3
PHASES = TICKS + 2

NORM_EPS = 1e-05
CHUNKS = 1


def shifted(value, axis, steps):
    count = lax.axis_size(axis)
    pairs = [(source, (source + steps) % count) for source in range(count)]
    return lax.ppermute(value, axis, pairs)


def moved(value, axis, parity, drop=False):
    count = lax.axis_size(axis)
    pairs = [((target - 2) % count, target) for target in range(count) if target % 2 == parity]
    if drop:
        pairs = [pair for pair in pairs if pair[1] != 1]
    return lax.ppermute(value, axis, pairs)


def swapped(value, axis):
    return lax.ppermute(value, axis, [(s, s + 1 - 2 * (s % 2)) for s in range(lax.axis_size(axis))])


def exchange(blocks, axis):
    return lax.all_to_all(blocks, axis, split_axis=0, concat_axis=0, tiled=True)


def head_context(block_of, count, breadth, gain_of, weights_of, normed_ref, centered_ref):
    features = count * breadth
    step = features // CHUNKS
    rows = normed_ref.shape[0]

    def row_sums(values_of):
        total = jnp.zeros((rows, HD), jnp.float32)
        for b in range(count):
            value = values_of(b)
            total = total + sum(value[:, c * HD : (c + 1) * HD] for c in range(breadth // HD))
        return jnp.sum(total, axis=-1, keepdims=True)

    mean = row_sums(block_of) * (1.0 / features)

    def squares(b):
        centered = block_of(b) - mean
        centered_ref[:, b * breadth : (b + 1) * breadth] = centered
        return centered * centered

    var = row_sums(squares) * (1.0 / features)
    scale = lax.rsqrt(var + NORM_EPS)
    for b in range(count):
        gain = gain_of(b).astype(jnp.float32)
        normed_ref[:, b * breadth : (b + 1) * breadth] = (centered_ref[:, b * breadth : (b + 1) * breadth] * scale * gain).astype(
            jnp.bfloat16
        )
    projected = jnp.zeros((rows, 3 * HD), jnp.float32)
    for c in range(CHUNKS):
        w_ref = weights_of(c)
        side_by_side = jnp.concatenate([w_ref[j, c * step : (c + 1) * step, :] for j in range(3)], axis=1)
        projected = projected + jnp.dot(
            normed_ref[:, c * step : (c + 1) * step], side_by_side, preferred_element_type=jnp.float32
        )
    projected = projected.astype(jnp.bfloat16)
    queries, keys, values = projected[:, :HD], projected[:, HD : 2 * HD], projected[:, 2 * HD :]
    scores = lax.dot_general(
        queries, keys, (((1,), (1,)), ((), ())), preferred_element_type=jnp.float32
    ) * HD ** (-0.5)
    causal = lax.broadcasted_iota(jnp.int32, scores.shape, 0) >= lax.broadcasted_iota(
        jnp.int32, scores.shape, 1
    )
    scores = jnp.where(causal, scores, -jnp.inf)
    weights = jnp.exp(scores - jnp.max(scores, axis=-1, keepdims=True))
    probs = (weights / jnp.sum(weights, axis=-1, keepdims=True)).astype(jnp.bfloat16)
    return jnp.dot(probs, values, preferred_element_type=jnp.float32).astype(jnp.bfloat16)


def opening_kernel(
    lost_hbm, plan_hbm, x_hbm, gain_hbm, w_hbm, mix_hbm, out_ref, x_sh_ref, facts_ref, x_ref, gain_ref, normed_ref, centered_ref, w_ref, lost_ref, plan_ref, sems, x_sems, w_sems, mix_sems
):
    count = out_ref.shape[0]
    rows, features = x_ref.shape
    breadth = features // count
    step = features // CHUNKS
    x_copies = [
        pltpu.make_async_copy(
            x_hbm.at[:, pl.ds(c * step, step)], x_ref.at[:, pl.ds(c * step, step)], x_sems.at[c]
        )
        for c in range(CHUNKS)
    ]
    gain_copy = pltpu.make_async_copy(gain_hbm, gain_ref, sems.at[0])
    lost_copy = pltpu.make_async_copy(lost_hbm, lost_ref, sems.at[1])
    plan_copy = pltpu.make_async_copy(plan_hbm, plan_ref, sems.at[2])
    w_copies = [
        pltpu.make_async_copy(
            w_hbm.at[:, pl.ds(c * step, step), :], w_ref.at[:, pl.ds(c * step, step), :], w_sems.at[c]
        )
        for c in range(CHUNKS)
    ]
    mix_copies = [
        pltpu.make_async_copy(
            mix_hbm.at[:, pl.ds(b * breadth, breadth)], out_ref.at[b, :, pl.ds(0, breadth)], mix_sems.at[b]
        )
        for b in range(count)
    ]
    for copy in [lost_copy, plan_copy, *x_copies, gain_copy, *w_copies, *mix_copies]:
        copy.start()
    lost_copy.wait()
    plan_copy.wait()
    facts_ref[0] = lost_ref[0]
    for t in range(TICKS):
        facts_ref[t + 1] = plan_ref[t]
    dead = lost_ref[0] == lax.axis_index("section")

    def block_of(b):
        block = x_ref[:, b * breadth : (b + 1) * breadth].astype(jnp.float32)
        return jnp.where(dead, 0.0, block)

    def weights_of(c):
        w_copies[c].wait()
        return w_ref

    def gain_of(b):
        return gain_ref[:, b * breadth : (b + 1) * breadth]

    for copy in [*x_copies, gain_copy]:
        copy.wait()
    context = head_context(block_of, count, breadth, gain_of, weights_of, normed_ref, centered_ref)
    for b in range(count):
        out_ref[b, :, breadth:] = context
    start = pl.multiple_of(lax.axis_index("tp") * breadth, breadth)
    x_sh = x_ref[:, pl.ds(start, breadth)]
    x_sh_ref[...] = jnp.where(dead, jnp.zeros_like(x_sh), x_sh)
    for copy in mix_copies:
        copy.wait()


def phase_kernel(x_ref, pack_ref, w_ref, out_ref, normed_ref, centered_ref):
    count, _, breadth = x_ref.shape

    def gain_of(b):
        return pack_ref[count, b : b + 1, :]

    context = head_context(
        lambda b: x_ref[b].astype(jnp.float32), count, breadth, gain_of, lambda c: w_ref, normed_ref, centered_ref
    )
    for b in range(count):
        out_ref[b] = context


def mix_kernel(x_ref, heads_ref, mixed_ref, out_ref):
    branch = jnp.zeros(x_ref.shape, jnp.float32)
    for h in range(heads_ref.shape[0]):
        branch = branch + jnp.dot(heads_ref[h], mixed_ref[h], preferred_element_type=jnp.float32)
    out_ref[...] = (x_ref[...].astype(jnp.float32) + branch).astype(jnp.bfloat16)


def first_mix_kernel(x_ref, joint_ref, gain_ref, out_ref, pack_ref):
    count, breadth = joint_ref.shape[0], x_ref.shape[1]
    branch = jnp.zeros(x_ref.shape, jnp.float32)
    for h in range(count):
        branch = branch + jnp.dot(
            joint_ref[h, :, breadth:], joint_ref[h, :, :breadth], preferred_element_type=jnp.float32
        )
    out_ref[...] = (x_ref[...].astype(jnp.float32) + branch).astype(jnp.bfloat16)
    for h in range(count):
        pack_ref[h] = joint_ref[h, :, :breadth]
    pack_ref[count] = jnp.zeros(x_ref.shape, jnp.bfloat16)
    for b in range(count):
        pack_ref[count, b : b + 1] = gain_ref[:, b * breadth : (b + 1) * breadth]


def lost_near_end(lost, sections):
    return (lost == sections - 2) | (lost == sections - 3)


def enter_kernel(following, facts_ref, moved_ref, stayed_ref, pool_ref, kept_ref, x_ref, copies_ref, keep_ref):
    sections, mine, lost = lax.axis_size("section"), lax.axis_index("section"), facts_ref[0]
    late = lost_near_end(lost, sections)
    phase = following - 1
    rows = jnp.where(mine % 2 == phase % 2, moved_ref[...], stayed_ref[...])
    if keep_ref is not None:
        before = (mine + sections - 1) % sections
        ahead = before - lost
        if phase == 2:
            here = (before != 0) & (ahead == 1)
        else:
            here = jnp.where(before == 0, ~late, (ahead < 1) | (ahead > 3))
        kept = jnp.zeros_like(rows) if kept_ref is None else kept_ref[...]
        keep_ref[...] = jnp.where(here, rows, kept)
    first = mine == (0 if following % 2 == 1 else 1)
    if following == 4:
        first = first & late
    if following == 5:
        first = first & ~late
    rows = jnp.where(first, pool_ref[facts_ref[min(following - 1, TICKS)]], rows)
    if following == 3:
        rows = jnp.where((mine == lost) & (lost == sections - 1), jnp.zeros_like(rows), rows)
    x_ref[...] = rows
    for b in range(copies_ref.shape[0]):
        copies_ref[b] = rows


def later_kernel(facts_ref, fifth_ref, fourth_ref, out_ref):
    sections, mine, lost = lax.axis_size("section"), lax.axis_index("section"), facts_ref[0]
    count, _, breadth = fifth_ref.shape
    behind = mine - lost
    late = lost_near_end(lost, sections)
    second = ((mine == 0) & ~late) | ((mine != 0) & (behind >= 1) & (behind <= 3))

    def store(block_of):
        for b in range(count):
            out_ref[:, b * breadth : (b + 1) * breadth] = block_of(b)

    @pl.when(mine == lost)
    def _():
        store(lambda b: jnp.zeros(fifth_ref.shape[1:], jnp.bfloat16))

    @pl.when((mine != lost) & second)
    def _():
        store(lambda b: fifth_ref[b])

    @pl.when((mine != lost) & ~second)
    def _():
        store(lambda b: fourth_ref[b])


def standby_kernel(facts_ref, arrived_ref, kept_ref, out_ref):
    sections, mine, lost = lax.axis_size("section"), lax.axis_index("section"), facts_ref[0]
    before = (mine + sections - 1) % sections
    ahead = before - lost
    here = ((before == 0) & lost_near_end(lost, sections)) | ((before != 0) & (ahead >= 2) & (ahead <= 3))
    out_ref[...] = jnp.where(here, arrived_ref[...], kept_ref[...])


VMEM = pl.BlockSpec(memory_space=pltpu.VMEM)
SMEM = pl.BlockSpec(memory_space=pltpu.SMEM)
HBM = pl.BlockSpec(memory_space=pltpu.HBM)
LIMIT = pltpu.CompilerParams(vmem_limit_bytes=16 * 1024 * 1024)
WHOLE = pltpu.CompilerParams(vmem_limit_bytes=57 * 1024 * 1024)


def opening(lost, plan, x_full, gain, w_in, mixing, members):
    rows, features = x_full.shape
    breadth = features // members
    return pl.pallas_call(
        opening_kernel,
        out_shape=[
            pltpu.VMEM((members, rows, breadth + HD), jnp.bfloat16),
            pltpu.VMEM((rows, breadth), jnp.bfloat16),
            pltpu.SMEM((TICKS + 1,), jnp.int32),
        ],
        in_specs=[HBM] * 6,
        out_specs=[VMEM, VMEM, SMEM],
        scratch_shapes=[
            pltpu.VMEM((rows, features), jnp.bfloat16),
            pltpu.VMEM((1, features), jnp.bfloat16),
            pltpu.VMEM((rows, features), jnp.bfloat16),
            pltpu.VMEM((rows, features), jnp.float32),
            pltpu.VMEM((3, features, HD), jnp.bfloat16),
            pltpu.SMEM(lost.shape, jnp.int32),
            pltpu.SMEM(plan.shape, jnp.int32),
            pltpu.SemaphoreType.DMA((3,)),
            pltpu.SemaphoreType.DMA((CHUNKS,)),
            pltpu.SemaphoreType.DMA((CHUNKS,)),
            pltpu.SemaphoreType.DMA((members,)),
        ],
        compiler_params=WHOLE,
        name="opening",
    )(lost, plan, x_full, gain, w_in, mixing)


def contexts(x_blocks, pack, w_in):
    members, rows, breadth = x_blocks.shape
    return pl.pallas_call(
        phase_kernel,
        out_shape=jax.ShapeDtypeStruct((members, rows, HD), jnp.bfloat16),
        in_specs=[VMEM, VMEM, VMEM],
        out_specs=VMEM,
        scratch_shapes=[
            pltpu.VMEM((rows, members * breadth), jnp.bfloat16),
            pltpu.VMEM((rows, members * breadth), jnp.float32),
        ],
        compiler_params=LIMIT,
        name="contexts",
    )(x_blocks, pack, w_in)


def mixed_rows(x_sh, heads, mixed):
    return pl.pallas_call(
        mix_kernel,
        out_shape=jax.ShapeDtypeStruct(x_sh.shape, jnp.bfloat16),
        in_specs=[VMEM, VMEM, VMEM],
        out_specs=VMEM,
        compiler_params=LIMIT,
        name="mixed_rows",
    )(x_sh, heads, mixed)


def first_mixed_rows(x_sh, joint, gain):
    members, rows, _ = joint.shape
    return pl.pallas_call(
        first_mix_kernel,
        out_shape=[
            jax.ShapeDtypeStruct(x_sh.shape, jnp.bfloat16),
            jax.ShapeDtypeStruct((members + 1, rows, x_sh.shape[1]), jnp.bfloat16),
        ],
        in_specs=[VMEM, VMEM, VMEM],
        out_specs=[VMEM, VMEM],
        compiler_params=LIMIT,
        name="first_mixed_rows",
    )(x_sh, joint, gain)


def entering_rows(following, facts, moved_rows, stayed_rows, pool, kept, members):
    keeps = following % 2 == 1
    operands = [facts, moved_rows, stayed_rows, pool]
    if kept is not None:
        operands.append(kept)
    shape = jax.ShapeDtypeStruct(stayed_rows.shape, jnp.bfloat16)
    copies = jax.ShapeDtypeStruct((members, *stayed_rows.shape), jnp.bfloat16)

    def body(*refs):
        inputs, outputs = list(refs[: len(operands)]), list(refs[len(operands) :])
        if kept is None:
            inputs.append(None)
        if not keeps:
            outputs.append(None)
        enter_kernel(following, *inputs, *outputs)

    return pl.pallas_call(
        body,
        out_shape=[shape, copies] + [shape] * keeps,
        in_specs=[SMEM] + [VMEM] * (len(operands) - 1),
        out_specs=[VMEM] * (2 + keeps),
        compiler_params=LIMIT,
        name="entering_rows",
    )(*operands)


def later_rows(facts, fifth, fourth):
    members, rows, breadth = fifth.shape
    return pl.pallas_call(
        later_kernel,
        out_shape=jax.ShapeDtypeStruct((rows, members * breadth), jnp.bfloat16),
        in_specs=[SMEM, VMEM, VMEM],
        out_specs=VMEM,
        compiler_params=LIMIT,
        name="later_rows",
    )(facts, fifth, fourth)


def standby_rows(facts, arrived, kept):
    return pl.pallas_call(
        standby_kernel,
        out_shape=jax.ShapeDtypeStruct(kept.shape, jnp.bfloat16),
        in_specs=[SMEM, VMEM, VMEM],
        out_specs=VMEM,
        compiler_params=LIMIT,
        name="standby_rows",
    )(facts, arrived, kept)


def per_device(
    pending_activation,
    admissible_microbatches,
    arrival_plan,
    vanished_hop,
    query_key_value_matrices,
    mixing_projection_matrices,
    normalizer_factors,
):
    members = lax.axis_size("tp")
    w_in = jnp.moveaxis(query_key_value_matrices[0], 1, 0)
    other_w = swapped(w_in, "section")
    sent, x_sh, facts = opening(
        vanished_hop,
        arrival_plan,
        pending_activation[0],
        normalizer_factors,
        w_in,
        mixing_projection_matrices[0],
        members,
    )
    y_sh, pack = first_mixed_rows(x_sh, exchange(sent, "tp"), normalizer_factors)
    other_pack = swapped(pack, "section")

    kept = None
    for following in range(2, PHASES + 1):
        moved_rows = moved(y_sh, "section", (following - 1) % 2, following == 2)
        x_sh, copies, *keep = entering_rows(
            following, facts, moved_rows, y_sh, admissible_microbatches, kept, members
        )
        if keep:
            kept = keep[0]
        if following == PHASES:
            copies, fourth = lax.optimization_barrier((copies, fourth))
        x_blocks = exchange(copies, "tp")
        if following == PHASES - 1:
            fourth = swapped(x_blocks, "section")
        layer_w, layer_pack = (w_in, pack) if following % 2 == 1 else (other_w, other_pack)
        heads = exchange(contexts(x_blocks, layer_pack, layer_w), "tp")
        y_sh = mixed_rows(x_sh, heads, layer_pack)
    y_sh, x_blocks, fourth = lax.optimization_barrier((y_sh, x_blocks, fourth))
    arrived = shifted(y_sh, "section", 1)
    later = later_rows(facts, x_blocks, fourth)
    return (later[None], standby_rows(facts, arrived, kept)[None])


def solution(mesh):
    placed = (
        P("section", None, None),
        P(None, None, "tp"),
        P(),
        P(),
        P("section", None, None, "tp"),
        P("section", "tp", None),
        P("section", None),
    )
    return jax.shard_map(
        per_device,
        mesh=mesh,
        in_specs=placed,
        out_specs=(P("section", None, None), P("section", None, "tp")),
        check_vma=False,
    )
```

```python
import jax
import jax.numpy as jnp
from jax import lax
from jax.experimental import pallas as pl
from jax.experimental.pallas import tpu as pltpu
from jax.sharding import PartitionSpec as P

HD = 128
TICKS = 3
PHASES = TICKS + 2

NORM_EPS = 1e-05
CHUNKS = 1


def shifted(value, axis, steps):
    count = lax.axis_size(axis)
    pairs = [(source, (source + steps) % count) for source in range(count)]
    return lax.ppermute(value, axis, pairs)


def moved(value, axis, parity):
    count = lax.axis_size(axis)
    pairs = [((t - 2) % count if t % 2 == parity else t, t) for t in range(count)]
    return lax.ppermute(value, axis, pairs)


def swapped(value, axis):
    return lax.ppermute(value, axis, [(s, s + 1 - 2 * (s % 2)) for s in range(lax.axis_size(axis))])


def exchange(blocks, axis):
    return lax.all_to_all(blocks, axis, split_axis=0, concat_axis=0, tiled=True)


def head_context(block_of, count, breadth, gain_of, weights_of, normed_ref, centered_ref):
    features = count * breadth
    step = features // CHUNKS
    rows = normed_ref.shape[0]

    def row_sums(values_of):
        total = jnp.zeros((rows, HD), jnp.float32)
        for b in range(count):
            value = values_of(b)
            total = total + sum(value[:, c * HD : (c + 1) * HD] for c in range(breadth // HD))
        return jnp.sum(total, axis=-1, keepdims=True)

    mean = row_sums(block_of) * (1.0 / features)

    def squares(b):
        centered = block_of(b) - mean
        centered_ref[:, b * breadth : (b + 1) * breadth] = centered
        return centered * centered

    var = row_sums(squares) * (1.0 / features)
    scale = lax.rsqrt(var + NORM_EPS)
    for b in range(count):
        gain = gain_of(b).astype(jnp.float32)
        normed_ref[:, b * breadth : (b + 1) * breadth] = (centered_ref[:, b * breadth : (b + 1) * breadth] * scale * gain).astype(
            jnp.bfloat16
        )
    projected = jnp.zeros((rows, 3 * HD), jnp.float32)
    for c in range(CHUNKS):
        w_ref = weights_of(c)
        side_by_side = jnp.concatenate([w_ref[j, c * step : (c + 1) * step, :] for j in range(3)], axis=1)
        projected = projected + jnp.dot(
            normed_ref[:, c * step : (c + 1) * step], side_by_side, preferred_element_type=jnp.float32
        )
    projected = projected.astype(jnp.bfloat16)
    queries, keys, values = projected[:, :HD], projected[:, HD : 2 * HD], projected[:, 2 * HD :]
    scores = lax.dot_general(
        queries, keys, (((1,), (1,)), ((), ())), preferred_element_type=jnp.float32
    ) * HD ** (-0.5)
    causal = lax.broadcasted_iota(jnp.int32, scores.shape, 0) >= lax.broadcasted_iota(
        jnp.int32, scores.shape, 1
    )
    scores = jnp.where(causal, scores, -jnp.inf)
    weights = jnp.exp(scores - jnp.max(scores, axis=-1, keepdims=True))
    probs = (weights / jnp.sum(weights, axis=-1, keepdims=True)).astype(jnp.bfloat16)
    return jnp.dot(probs, values, preferred_element_type=jnp.float32).astype(jnp.bfloat16)


def opening_kernel(
    lost_hbm, plan_hbm, x_hbm, gain_hbm, w_hbm, mix_hbm, out_ref, x_sh_ref, facts_ref, x_ref, gain_ref, normed_ref, centered_ref, w_ref, lost_ref, plan_ref, sems, x_sems, w_sems, mix_sems
):
    count = out_ref.shape[0]
    rows, features = x_ref.shape
    breadth = features // count
    step = features // CHUNKS
    x_copies = [
        pltpu.make_async_copy(
            x_hbm.at[:, pl.ds(c * step, step)], x_ref.at[:, pl.ds(c * step, step)], x_sems.at[c]
        )
        for c in range(CHUNKS)
    ]
    gain_copy = pltpu.make_async_copy(gain_hbm, gain_ref, sems.at[0])
    lost_copy = pltpu.make_async_copy(lost_hbm, lost_ref, sems.at[1])
    plan_copy = pltpu.make_async_copy(plan_hbm, plan_ref, sems.at[2])
    w_copies = [
        pltpu.make_async_copy(
            w_hbm.at[:, pl.ds(c * step, step), :], w_ref.at[:, pl.ds(c * step, step), :], w_sems.at[c]
        )
        for c in range(CHUNKS)
    ]
    mix_copies = [
        pltpu.make_async_copy(
            mix_hbm.at[:, pl.ds(b * breadth, breadth)], out_ref.at[b, :, pl.ds(0, breadth)], mix_sems.at[b]
        )
        for b in range(count)
    ]
    for copy in [lost_copy, plan_copy, *x_copies, gain_copy, *w_copies, *mix_copies]:
        copy.start()
    lost_copy.wait()
    plan_copy.wait()
    facts_ref[0] = lost_ref[0]
    for t in range(TICKS):
        facts_ref[t + 1] = plan_ref[t]
    dead = lost_ref[0] == lax.axis_index("section")

    def block_of(b):
        block = x_ref[:, b * breadth : (b + 1) * breadth].astype(jnp.float32)
        return jnp.where(dead, 0.0, block)

    def weights_of(c):
        w_copies[c].wait()
        return w_ref

    def gain_of(b):
        return gain_ref[:, b * breadth : (b + 1) * breadth]

    for copy in [*x_copies, gain_copy]:
        copy.wait()
    context = head_context(block_of, count, breadth, gain_of, weights_of, normed_ref, centered_ref)
    for b in range(count):
        out_ref[b, :, breadth:] = context
    start = pl.multiple_of(lax.axis_index("tp") * breadth, breadth)
    x_sh = x_ref[:, pl.ds(start, breadth)]
    x_sh_ref[...] = jnp.where(dead, jnp.zeros_like(x_sh), x_sh)
    for copy in mix_copies:
        copy.wait()


def phase_kernel(x_ref, pack_ref, w_ref, out_ref, normed_ref, centered_ref):
    count, _, breadth = x_ref.shape

    def gain_of(b):
        return pack_ref[count, b : b + 1, :]

    context = head_context(
        lambda b: x_ref[b].astype(jnp.float32), count, breadth, gain_of, lambda c: w_ref, normed_ref, centered_ref
    )
    for b in range(count):
        out_ref[b] = context


def mix_kernel(x_ref, heads_ref, mixed_ref, out_ref):
    branch = jnp.zeros(x_ref.shape, jnp.float32)
    for h in range(heads_ref.shape[0]):
        branch = branch + jnp.dot(heads_ref[h], mixed_ref[h], preferred_element_type=jnp.float32)
    out_ref[...] = (x_ref[...].astype(jnp.float32) + branch).astype(jnp.bfloat16)


def first_mix_kernel(x_ref, joint_ref, gain_ref, out_ref, pack_ref):
    count, breadth = joint_ref.shape[0], x_ref.shape[1]
    branch = jnp.zeros(x_ref.shape, jnp.float32)
    for h in range(count):
        branch = branch + jnp.dot(
            joint_ref[h, :, breadth:], joint_ref[h, :, :breadth], preferred_element_type=jnp.float32
        )
    out_ref[...] = (x_ref[...].astype(jnp.float32) + branch).astype(jnp.bfloat16)
    for h in range(count):
        pack_ref[h] = joint_ref[h, :, :breadth]
    pack_ref[count] = jnp.zeros(x_ref.shape, jnp.bfloat16)
    for b in range(count):
        pack_ref[count, b : b + 1] = gain_ref[:, b * breadth : (b + 1) * breadth]


def lost_near_end(lost, sections):
    return (lost == sections - 2) | (lost == sections - 3)


def enter_kernel(following, facts_ref, moved_ref, stayed_ref, pool_ref, kept_ref, x_ref, copies_ref, keep_ref):
    sections, mine, lost = lax.axis_size("section"), lax.axis_index("section"), facts_ref[0]
    late = lost_near_end(lost, sections)
    phase = following - 1
    rows = moved_ref[...]
    if keep_ref is not None:
        before = (mine + sections - 1) % sections
        ahead = before - lost
        if phase == 2:
            here = (before != 0) & (ahead == 1)
        else:
            here = jnp.where(before == 0, ~late, (ahead < 1) | (ahead > 3))
        kept = jnp.zeros_like(rows) if kept_ref is None else kept_ref[...]
        keep_ref[...] = jnp.where(here, rows, kept)
    first = mine == (0 if following % 2 == 1 else 1)
    if following == 4:
        first = first & late
    if following == 5:
        first = first & ~late
    rows = jnp.where(first, pool_ref[facts_ref[min(following - 1, TICKS)]], rows)
    if following == 3:
        rows = jnp.where((mine == lost) & (lost == sections - 1), jnp.zeros_like(rows), rows)
    x_ref[...] = rows
    for b in range(copies_ref.shape[0]):
        copies_ref[b] = rows


def later_kernel(facts_ref, fifth_ref, fourth_ref, out_ref):
    sections, mine, lost = lax.axis_size("section"), lax.axis_index("section"), facts_ref[0]
    count, _, breadth = fifth_ref.shape
    behind = mine - lost
    late = lost_near_end(lost, sections)
    second = ((mine == 0) & ~late) | ((mine != 0) & (behind >= 1) & (behind <= 3))

    def store(block_of):
        for b in range(count):
            out_ref[:, b * breadth : (b + 1) * breadth] = block_of(b)

    @pl.when(mine == lost)
    def _():
        store(lambda b: jnp.zeros(fifth_ref.shape[1:], jnp.bfloat16))

    @pl.when((mine != lost) & second)
    def _():
        store(lambda b: fifth_ref[b])

    @pl.when((mine != lost) & ~second)
    def _():
        store(lambda b: fourth_ref[b])


def standby_kernel(facts_ref, arrived_ref, kept_ref, out_ref):
    sections, mine, lost = lax.axis_size("section"), lax.axis_index("section"), facts_ref[0]
    before = (mine + sections - 1) % sections
    ahead = before - lost
    here = ((before == 0) & lost_near_end(lost, sections)) | ((before != 0) & (ahead >= 2) & (ahead <= 3))
    out_ref[...] = jnp.where(here, arrived_ref[...], kept_ref[...])


VMEM = pl.BlockSpec(memory_space=pltpu.VMEM)
SMEM = pl.BlockSpec(memory_space=pltpu.SMEM)
HBM = pl.BlockSpec(memory_space=pltpu.HBM)
LIMIT = pltpu.CompilerParams(vmem_limit_bytes=16 * 1024 * 1024)
WHOLE = pltpu.CompilerParams(vmem_limit_bytes=57 * 1024 * 1024)


def opening(lost, plan, x_full, gain, w_in, mixing, members):
    rows, features = x_full.shape
    breadth = features // members
    return pl.pallas_call(
        opening_kernel,
        out_shape=[
            pltpu.VMEM((members, rows, breadth + HD), jnp.bfloat16),
            pltpu.VMEM((rows, breadth), jnp.bfloat16),
            pltpu.SMEM((TICKS + 1,), jnp.int32),
        ],
        in_specs=[HBM] * 6,
        out_specs=[VMEM, VMEM, SMEM],
        scratch_shapes=[
            pltpu.VMEM((rows, features), jnp.bfloat16),
            pltpu.VMEM((1, features), jnp.bfloat16),
            pltpu.VMEM((rows, features), jnp.bfloat16),
            pltpu.VMEM((rows, features), jnp.float32),
            pltpu.VMEM((3, features, HD), jnp.bfloat16),
            pltpu.SMEM(lost.shape, jnp.int32),
            pltpu.SMEM(plan.shape, jnp.int32),
            pltpu.SemaphoreType.DMA((3,)),
            pltpu.SemaphoreType.DMA((CHUNKS,)),
            pltpu.SemaphoreType.DMA((CHUNKS,)),
            pltpu.SemaphoreType.DMA((members,)),
        ],
        compiler_params=WHOLE,
        name="opening",
    )(lost, plan, x_full, gain, w_in, mixing)


def contexts(x_blocks, pack, w_in):
    members, rows, breadth = x_blocks.shape
    return pl.pallas_call(
        phase_kernel,
        out_shape=jax.ShapeDtypeStruct((members, rows, HD), jnp.bfloat16),
        in_specs=[VMEM, VMEM, VMEM],
        out_specs=VMEM,
        scratch_shapes=[
            pltpu.VMEM((rows, members * breadth), jnp.bfloat16),
            pltpu.VMEM((rows, members * breadth), jnp.float32),
        ],
        compiler_params=LIMIT,
        name="contexts",
    )(x_blocks, pack, w_in)


def mixed_rows(x_sh, heads, mixed):
    return pl.pallas_call(
        mix_kernel,
        out_shape=jax.ShapeDtypeStruct(x_sh.shape, jnp.bfloat16),
        in_specs=[VMEM, VMEM, VMEM],
        out_specs=VMEM,
        compiler_params=LIMIT,
        name="mixed_rows",
    )(x_sh, heads, mixed)


def first_mixed_rows(x_sh, joint, gain):
    members, rows, _ = joint.shape
    return pl.pallas_call(
        first_mix_kernel,
        out_shape=[
            jax.ShapeDtypeStruct(x_sh.shape, jnp.bfloat16),
            jax.ShapeDtypeStruct((members + 1, rows, x_sh.shape[1]), jnp.bfloat16),
        ],
        in_specs=[VMEM, VMEM, VMEM],
        out_specs=[VMEM, VMEM],
        compiler_params=LIMIT,
        name="first_mixed_rows",
    )(x_sh, joint, gain)


def entering_rows(following, facts, moved_rows, stayed_rows, pool, kept, members):
    keeps = following % 2 == 1
    operands = [facts, moved_rows, stayed_rows, pool]
    if kept is not None:
        operands.append(kept)
    shape = jax.ShapeDtypeStruct(stayed_rows.shape, jnp.bfloat16)
    copies = jax.ShapeDtypeStruct((members, *stayed_rows.shape), jnp.bfloat16)

    def body(*refs):
        inputs, outputs = list(refs[: len(operands)]), list(refs[len(operands) :])
        if kept is None:
            inputs.append(None)
        if not keeps:
            outputs.append(None)
        enter_kernel(following, *inputs, *outputs)

    return pl.pallas_call(
        body,
        out_shape=[shape, copies] + [shape] * keeps,
        in_specs=[SMEM] + [VMEM] * (len(operands) - 1),
        out_specs=[VMEM] * (2 + keeps),
        compiler_params=LIMIT,
        name="entering_rows",
    )(*operands)


def later_rows(facts, fifth, fourth):
    members, rows, breadth = fifth.shape
    return pl.pallas_call(
        later_kernel,
        out_shape=jax.ShapeDtypeStruct((rows, members * breadth), jnp.bfloat16),
        in_specs=[SMEM, VMEM, VMEM],
        out_specs=VMEM,
        compiler_params=LIMIT,
        name="later_rows",
    )(facts, fifth, fourth)


def standby_rows(facts, arrived, kept):
    return pl.pallas_call(
        standby_kernel,
        out_shape=jax.ShapeDtypeStruct(kept.shape, jnp.bfloat16),
        in_specs=[SMEM, VMEM, VMEM],
        out_specs=VMEM,
        compiler_params=LIMIT,
        name="standby_rows",
    )(facts, arrived, kept)


def per_device(
    pending_activation,
    admissible_microbatches,
    arrival_plan,
    vanished_hop,
    query_key_value_matrices,
    mixing_projection_matrices,
    normalizer_factors,
):
    members = lax.axis_size("tp")
    w_in = jnp.moveaxis(query_key_value_matrices[0], 1, 0)
    other_w = swapped(w_in, "section")
    sent, x_sh, facts = opening(
        vanished_hop,
        arrival_plan,
        pending_activation[0],
        normalizer_factors,
        w_in,
        mixing_projection_matrices[0],
        members,
    )
    y_sh, pack = first_mixed_rows(x_sh, exchange(sent, "tp"), normalizer_factors)
    other_pack = swapped(pack, "section")

    kept = None
    for following in range(2, PHASES + 1):
        moved_rows = moved(y_sh, "section", (following - 1) % 2)
        x_sh, copies, *keep = entering_rows(
            following, facts, moved_rows, y_sh, admissible_microbatches, kept, members
        )
        if keep:
            kept = keep[0]
        if following == PHASES:
            copies, fourth = lax.optimization_barrier((copies, fourth))
        x_blocks = exchange(copies, "tp")
        if following == PHASES - 1:
            fourth = swapped(x_blocks, "section")
        layer_w, layer_pack = (w_in, pack) if following % 2 == 1 else (other_w, other_pack)
        heads = exchange(contexts(x_blocks, layer_pack, layer_w), "tp")
        y_sh = mixed_rows(x_sh, heads, layer_pack)
    y_sh, x_blocks, fourth = lax.optimization_barrier((y_sh, x_blocks, fourth))
    arrived = shifted(y_sh, "section", 1)
    later = later_rows(facts, x_blocks, fourth)
    return (later[None], standby_rows(facts, arrived, kept)[None])


def solution(mesh):
    placed = (
        P("section", None, None),
        P(None, None, "tp"),
        P(),
        P(),
        P("section", None, None, "tp"),
        P("section", "tp", None),
        P("section", None),
    )
    return jax.shard_map(
        per_device,
        mesh=mesh,
        in_specs=placed,
        out_specs=(P("section", None, None), P("section", None, "tp")),
        check_vma=False,
    )
```
